256 devices in a mesh: row: 16 (over y, x), col: 16 (over z, core).
Axes of the slice: x: 4, y: 4, z: 8, core: 2. Of those that a mesh axis runs over, the one named last changes fastest.
Arguments:
- matrix: float32 [3, 16, 256, 3, 16, 256], P(None, 'row', None, None, 'col'), may hold values from -1.4 to 1.4, as said below
- vectors: float32 [4096, 3, 16, 256], P('col', None, 'row'), may hold values from -6 to 6
Outputs:
- reduced: float32 [3, 16, 256, 3, 16, 256], P(None, 'row', None, None, 'col')
- transformed: float32 [4096, 3, 16, 256], P('col', None, 'row')
The draws below stay inside these ranges and needn't reach their ends.
Inputs may be any that keep to these rules, and one draw needn't show every extreme that they name: `matrix`: symmetric as the 12288 x 12288 array of its meaning.
All inputs are finite; a program needn't handle non-finite values.
Results may differ from the reference program's by a relative error of at most 0.00013.
Values sent between devices are 32-bit elements; how exact they have to be, the bound alone decides.
A program may use at most 128 MiB of HBM per device.

```python
import jax
import jax.numpy as jnp
from jax import lax

ORDER = 12288
BAND = 256
PANELS = 1
GRID_ROWS = 16
GRID_COLS = 16
ROW_SLOTS = 3
COL_SLOTS = 3
VEC_ROWS = 4096


def draw_matrix(key, part):
    base_draw = jnp.clip(jax.random.normal(jax.random.fold_in(key, 13), (ORDER, ORDER), jnp.float32), -4.0, 4.0)
    symmetric = (base_draw + base_draw.T) * 0.1
    return symmetric.reshape(ROW_SLOTS, GRID_ROWS, BAND, COL_SLOTS, GRID_COLS, BAND)


def level_of(stream_key, dims, shards, least, top_value):
    level, own = 1.0, jax.random.fold_in(stream_key, 6)
    for axis_at, shards_of in shards:
        heights = jnp.exp(jax.random.uniform(jax.random.fold_in(own, axis_at), (shards_of,), jnp.float32, least / len(shards), top_value / len(shards)))
        level = level * jnp.repeat(heights, dims[axis_at] // shards_of).reshape([-1 if axis == axis_at else 1 for axis in range(len(dims))])
    return level


def normal_values(key, extent, deviation, reach, pieces=(), kind=jnp.bfloat16):
    entries = deviation * jax.random.normal(key, extent, jnp.float32)
    if pieces:
        entries = entries * level_of(key, extent, pieces, -0.22, 0.18)
    return jnp.clip(entries, -reach, reach).astype(kind)


def setup_inputs(seed: int = 0) -> dict:
    key_of = jax.random.split(jax.random.key(seed), 3)
    matrix = draw_matrix(jax.random.fold_in(key_of[2], 71), 0)
    vectors = normal_values(key_of[1], (VEC_ROWS, ROW_SLOTS, GRID_ROWS, BAND), 1.0, 6.0, ((0, 16), (2, 16)), jnp.float32)
    return dict(matrix=matrix, vectors=vectors)


precise = lax.Precision.HIGHEST

def matmul(left_side, right_side):
    return jnp.dot(left_side.astype(jnp.float32), right_side.astype(jnp.float32), precision=precise, preferred_element_type=jnp.float32)

def reference(matrix, vectors):
    current = matrix.reshape(ORDER, ORDER)
    projected_rows = vectors.reshape(VEC_ROWS, ORDER)
    identity = jnp.eye(BAND, dtype=jnp.float32)
    for panel_index in range(PANELS):
        begin = (panel_index + 1) * BAND
        panel_rows = current[begin:, panel_index * BAND:begin]
        gram_full = matmul(panel_rows.T, panel_rows)
        lower_factor = jnp.linalg.cholesky(gram_full)
        basis_rows = jax.scipy.linalg.solve_triangular(lower_factor, panel_rows.T, lower=True).T
        kernel = jnp.linalg.inv(identity + basis_rows[:BAND])
        reflect_rows = jnp.concatenate([jnp.zeros((begin, BAND), jnp.float32), basis_rows.at[:BAND].add(identity)], axis=0)
        image_full = matmul(current, reflect_rows)
        inner_gram = matmul(reflect_rows.T, image_full)
        middle = matmul(matmul(kernel.T, inner_gram), kernel)
        update_rows = matmul(image_full, kernel) - 0.5 * matmul(reflect_rows, middle)
        left_side = jnp.concatenate([update_rows, reflect_rows], axis=1)
        right_side = jnp.concatenate([reflect_rows, update_rows], axis=1)
        current = current - matmul(left_side, right_side.T)
        product = matmul(projected_rows, reflect_rows)
        projected_rows = projected_rows - matmul(matmul(product, kernel), reflect_rows.T)
    return (current.reshape(matrix.shape), projected_rows.reshape(vectors.shape))
```

```python
import functools

import jax
import jax.numpy as jnp
from jax import lax
from jax.experimental import pallas as pl
from jax.experimental.pallas import tpu as pltpu
from jax.sharding import PartitionSpec as P

MESH = pl.DeviceIdType.MESH
F32 = jnp.float32
HIGH = lax.Precision.HIGH
HIGHEST = lax.Precision.HIGHEST
STEP = 32
GROUP = 8
WIDE = 6


def dot(a, b, ca, cb, precision=HIGH):
    return lax.dot_general(
        a, b, (((ca,), (cb,)), ((), ())), precision=precision, preferred_element_type=F32
    )


def send(src, dst, ssem, rsem, axis, to):
    return pltpu.make_async_remote_copy(
        src_ref=src, dst_ref=dst, send_sem=ssem, recv_sem=rsem, device_id={axis: to}, device_id_type=MESH
    )


def loop(n, body):
    lax.fori_loop(0, n, lambda k, c: (body(k), c)[1], 0)


def greet(rows, cols, p, q):
    barrier = pltpu.get_barrier_semaphore()

    def hello_row(k):
        pl.semaphore_signal(barrier, inc=1, device_id={"row": lax.rem(p + 1 + k, rows)}, device_id_type=MESH)

    def hello_col(k):
        pl.semaphore_signal(barrier, inc=1, device_id={"col": lax.rem(q + 1 + k, cols)}, device_id_type=MESH)

    loop(rows - 1, hello_row)
    loop(cols - 1, hello_col)
    return lambda: pl.semaphore_wait(barrier, rows + cols - 2)


class Fan:
    def __init__(self, axis, size, me, ssem, rsem, src, dst, recv=None):
        self.axis, self.size, self.me = axis, size, me
        self.ssem, self.rsem, self.src, self.dst = ssem, rsem, src, dst
        self.recv = recv

    def copy(self, k):
        to = lax.rem(self.me + 1 + k, self.size)
        return send(self.src(to), self.dst(self.me), self.ssem.at[k], self.rsem.at[self.me], self.axis, to)

    def start(self):
        loop(self.size - 1, lambda k: self.copy(k).start())

    def wait_recv(self):
        def one(k):
            at = lax.rem(self.me + 1 + k, self.size)
            ref = self.dst(at)
            send(ref, ref, self.ssem.at[k], self.rsem.at[at], self.axis, at).wait_recv()

        loop(self.size - 1, one)

    def wait_send(self):
        loop(self.size - 1, lambda k: self.copy(k).wait_send())


class Scatter:
    def __init__(self, axis, size, me, root, ssem, rsem, src, dst):
        self.axis, self.size, self.me, self.root = axis, size, me, root
        self.ssem, self.rsem, self.src, self.dst = ssem, rsem, src, dst

    def copy(self, k):
        to = lax.rem(self.me + 1 + k, self.size)
        return send(self.src(to), self.dst(to), self.ssem.at[k], self.rsem, self.axis, to)

    def start(self):
        loop(self.size - 1, lambda k: self.copy(k).start())

    def wait_recv(self):
        ref = self.dst(self.me)
        send(ref, ref, self.ssem.at[0], self.rsem, self.axis, self.root).wait_recv()

    def wait_send(self):
        loop(self.size - 1, lambda k: self.copy(k).wait_send())


class Chips:
    def __init__(self, cols, q, zs, zr, ss, sr, ref):
        self.chips, self.cols, self.q, self.ref = cols // 2, cols, q, ref
        self.z, self.c = q // 2, lax.rem(q, 2)
        self.zs, self.zr, self.ss, self.sr = zs, zr, ss, sr

    def along(self, k):
        z = lax.rem(self.z + 1 + k, self.chips)
        mine = self.ref.at[self.q]
        return send(mine, mine, self.zs.at[k], self.zr.at[self.z], "col", 2 * z + self.c)

    def across(self, z):
        piece = self.ref.at[2 * z + self.c]
        return send(piece, piece, self.ss.at[z], self.sr.at[z], "col", 2 * self.z + 1 - self.c)

    def start(self):
        loop(self.chips - 1, lambda k: self.along(k).start())
        self.across(self.z).start()

    def relay(self):
        def one(k):
            z = lax.rem(self.z + 1 + k, self.chips)
            piece = self.ref.at[2 * z + self.c]
            send(piece, piece, self.zs.at[k], self.zr.at[z], "col", 2 * z + self.c).wait_recv()
            self.across(z).start()

        loop(self.chips - 1, one)

    def finish(self):
        loop(self.chips - 1, lambda k: self.along(k).wait_send())

        def one(z):
            self.across(z).wait_send()
            piece = self.ref.at[2 * z + 1 - self.c]
            send(piece, piece, self.ss.at[z], self.sr.at[z], "col", 2 * self.z + 1 - self.c).wait_recv()

        loop(self.chips, one)


def total(ref):
    size = ref.shape[0]
    acc = ref[0]
    for i in range(1, size):
        acc = acc + ref[i]
    return acc


def splat_row(x, j):
    return jnp.broadcast_to(x[j : j + 1, :], x.shape)


def small_inverse(tile, off, chol):
    row = lax.broadcasted_iota(jnp.int32, tile.shape, 0)
    lane = lax.broadcasted_iota(jnp.int32, tile.shape, 1)
    inverse = jnp.where(row == lane, 1.0, 0.0).astype(F32)
    pivots = jnp.ones_like(tile)
    for g in range(0, STEP, GROUP):
        cols = [jnp.broadcast_to(tile[:, off + g + i : off + g + i + 1], tile.shape) for i in range(GROUP)]
        for i in range(GROUP):
            j = g + i
            pivot = splat_row(cols[i], j)
            scale = 1.0 / pivot
            if chol:
                m = jnp.where(row > j, cols[i] * scale, 0.0)
                pivots = jnp.where(row == j, pivot, pivots)
            else:
                m = jnp.where(row == j, 1.0 - scale, cols[i] * scale)
            for k in range(i + 1, GROUP):
                cols[k] = cols[k] - m * splat_row(cols[k], j)
            tile = tile - m * splat_row(tile, j)
            inverse = inverse - m * splat_row(inverse, j)
    if chol:
        inverse = inverse * lax.rsqrt(pivots)
    return inverse[:, :STEP]


def eliminate(work, out, chol, halfway=None):
    size = work.shape[0]
    lane = lax.broadcasted_iota(jnp.int32, (STEP, size), 1)
    row = lax.broadcasted_iota(jnp.int32, (STEP, size), 0)
    for at in range(0, size, STEP):
        end = at + STEP
        if halfway is not None and 2 * at == size:
            halfway()
        base = at // 128 * 128
        inverse = small_inverse(work[at:end, base : base + 128], at - base, chol)
        strip = jnp.where(
            (lane >= at) & (lane < end), jnp.where(lane - at == row, 1.0, 0.0), work[at:end, :]
        )
        strip = dot(inverse, strip, 1, 0, HIGHEST)
        if chol:
            out[at:end, :] = jnp.where(lane < end, strip, 0.0)
            spans = [(end, size)]
        else:
            spans = [(0, at), (end, size)]
        for lo, hi in spans:
            if lo == hi:
                continue
            side = work[lo:hi, at:end]
            if chol:
                side = dot(side, inverse, 1, 1, HIGHEST)
            wide = lax.broadcasted_iota(jnp.int32, (hi - lo, size), 1)
            rest = jnp.where((wide >= at) & (wide < end), 0.0, work[lo:hi, :])
            work[lo:hi, :] = rest - dot(side, strip, 1, 0, HIGHEST)
        if not chol:
            work[at:end, :] = strip


def identity(size):
    row = lax.broadcasted_iota(jnp.int32, (size, size), 0)
    return jnp.where(row == lax.broadcasted_iota(jnp.int32, (size, size), 1), 1.0, 0.0).astype(F32)


def strip_of(ref, start, count, at):
    return ref[pl.ds(start * WIDE + at, count, stride=WIDE), :]


def main_kernel(
    rows, cols, alin, zlin,
    y_out, yt_out, v_out, vt_out, c_out, t_out, k_out,
    a, z, panel, panel_t, gram, landed, g_out, top_out, rows_out, cols_out, work, w,
    v, v_half, v_sum, v_land, vt, vt_land, c, c_half, c_sum, c_land, c_row, t, t_land,
    *sems,
):
    sems = iter(sems)
    p, q = lax.axis_index("row"), lax.axis_index("col")
    met = greet(rows, cols, p, q)
    first = q == 0
    chips = cols // 2
    my_z, core = q // 2, lax.rem(q, 2)
    other = 2 * my_z + 1 - core
    height, band = panel.shape
    slab, piece = rows_out.shape[1], top_out.shape[1]

    row = lax.broadcasted_iota(jnp.int32, (height, 128), 0)
    for at in range(band // 128):
        panel[:, 128 * at : 128 * (at + 1)] = jnp.where((row < band) & (p == 0), 0.0, strip_of(alin, 0, height, at))
    gram[...] = dot(panel[...], panel[...], 0, 0, HIGHEST).reshape(gram.shape)
    for at in range(WIDE):
        part = strip_of(alin, 0, band, at)
        if at < band // 128:
            part = jnp.where(q == 0, 0.0, part)
        panel_t[:, :, 128 * at : 128 * (at + 1)] = part.reshape(rows, band // rows, 128)

    def top_piece(to):
        return panel.at[pl.ds(pl.multiple_of(to * piece, piece), piece), :]

    def row_piece(to):
        return panel.at[pl.ds(pl.multiple_of(to * slab, slab), slab), :]

    def fan(axis, size, me, src, dst):
        return Fan(axis, size, me, next(sems), next(sems), src, dst)

    def cut(axis, size, me, root, src, dst):
        return Scatter(axis, size, me, root, next(sems), next(sems), src, dst)

    def ring(ref):
        return Chips(cols, q, next(sems), next(sems), next(sems), next(sems), ref)

    reduce = fan("row", rows, p, lambda to: gram.at[to], lambda at: landed.at[at])
    g_wide = fan("row", rows, p, lambda to: g_out.at[p], lambda at: g_out.at[at])
    t_wide = fan("row", rows, p, lambda to: top_out.at[p], lambda at: top_out.at[at])
    c_wide = fan("row", rows, p, lambda to: cols_out.at[p], lambda at: cols_out.at[at])
    vt_cut = fan("row", rows, p, lambda to: vt.at[to], lambda at: vt_land.at[at])
    pt_cut = fan("row", rows, p, lambda to: t.at[to], lambda at: t_land.at[at])
    pc_wide = fan("row", rows, p, lambda to: c_row.at[p], lambda at: c_row.at[at])
    vt_all = fan("row", rows, p, lambda to: vt_out.at[p], lambda at: vt_out.at[at])
    pt_all = fan("row", rows, p, lambda to: t_out.at[p], lambda at: t_out.at[at])
    g_down = cut("col", cols, q, 0, lambda to: g_out.at[p], lambda to: g_out.at[p])
    t_cut = cut("row", rows, p, 1, top_piece, lambda to: top_out.at[to])
    t_down = cut("col", cols, q, 0, lambda to: top_out.at[p], lambda to: top_out.at[p])
    r_cut = cut("col", cols, q, 0, row_piece, lambda to: rows_out.at[to])
    c_cut = cut("row", rows, p, 0, lambda to: panel_t.at[to], lambda to: cols_out.at[to])
    r_wide, v_all, c_all = ring(rows_out), ring(v_out), ring(c_out)

    met()

    @pl.when(first)
    def _():
        reduce.start()

        @pl.when(p == 1)
        def _():
            t_cut.start()

        r_cut.start()

    @pl.when(p == 0)
    def _():
        c_cut.start()

    @pl.when(first)
    def _():
        landed[p] = gram[p]
        rows_out[0] = panel[:slab, :]

        @pl.when(p == 1)
        def _():
            top_out[1] = panel[piece : 2 * piece, :]

        reduce.wait_recv()
        g_out[p] = total(landed)
        g_down.start()

    @pl.when(p == 0)
    def _():
        cols_out[0] = panel_t[0]

    @pl.when(jnp.logical_not(first))
    def _():
        g_down.wait_recv()

    g_wide.start()

    @pl.when(jnp.logical_not(first))
    def _():
        r_cut.wait_recv()

    r_wide.start()

    @pl.when(p != 0)
    def _():
        c_cut.wait_recv()

    c_wide.start()

    @pl.when(first)
    def _():
        @pl.when(p != 1)
        def _():
            t_cut.wait_recv()

        t_down.start()

    @pl.when(jnp.logical_not(first))
    def _():
        t_down.wait_recv()

    t_wide.start()
    for at in range(WIDE):
        a[:, 128 * at : 128 * (at + 1)] = strip_of(alin, 0, height, at)
        z[:, 128 * at : 128 * (at + 1)] = strip_of(zlin, 0, z.shape[0], at)
    g_wide.wait_recv()

    work[...] = g_out[...].reshape(band, band)
    eliminate(work, w, True, r_wide.relay)

    c_wide.wait_recv()
    yt_out[...] = dot(w[...], cols_out[...].reshape(band, height), 1, 0)
    r_wide.finish()
    y_out[...] = dot(rows_out[...].reshape(height, band), w[...], 1, 1)

    @pl.when(p == 1)
    def _():
        y_out[:band, :] = y_out[:band, :] + identity(band)

    @pl.when(q == 1)
    def _():
        yt_out[:, :band] = yt_out[:, :band] + identity(band)

    vt[...] = dot(y_out[...], a[...], 0, 0).reshape(vt.shape)
    vt_cut.start()

    image = dot(a[...], yt_out[...], 1, 1)
    for i in range(cols):
        v[i % 2, i // 2] = image[i * slab : (i + 1) * slab, :]
    v_swap = send(v.at[1 - core], v_half, next(sems), next(sems), "col", other)
    v_swap.start()
    t[...] = dot(z[...], y_out[...], 1, 0).reshape(t.shape)
    pt_cut.start()
    inner = dot(y_out[...], image, 0, 0)
    for i in range(cols):
        c[i % 2, i // 2] = inner[i * piece : (i + 1) * piece, :]
    c_swap = send(c.at[1 - core], c_half, next(sems), next(sems), "col", other)
    c_swap.start()
    vt_land[p] = vt[p]
    t_land[p] = t[p]

    def along(src, land):
        ss, rs = next(sems), next(sems)

        def copy(k):
            to = lax.rem(my_z + 1 + k, chips)
            return send(src.at[to], land.at[my_z], ss.at[k], rs.at[my_z], "col", 2 * to + core)

        def recv(k):
            at = lax.rem(my_z + 1 + k, chips)
            send(src.at[at], land.at[at], ss.at[k], rs.at[at], "col", 2 * at + core).wait_recv()

        return copy, recv

    v_copy, v_recv = along(v_sum, v_land)
    c_copy, c_recv = along(c_sum, c_land)
    v_swap.wait_recv()

    def v_add(i):
        v_sum[i] = v[core, i] + v_half[i]

    loop(chips, v_add)
    loop(chips - 1, lambda k: v_copy(k).start())
    c_swap.wait_recv()

    def c_add(i):
        c_sum[i] = c[core, i] + c_half[i]

    loop(chips, c_add)
    loop(chips - 1, lambda k: c_copy(k).start())
    v_land[my_z] = v_sum[my_z]
    c_land[my_z] = c_sum[my_z]

    t_wide.wait_recv()
    k_out[...] = identity(band) + dot(top_out[...].reshape(band, band), w[...], 1, 1, HIGHEST)
    eliminate(k_out, None, False)

    loop(chips - 1, c_recv)
    c_row[p] = total(c_land)
    pc_wide.start()

    vt_cut.wait_recv()
    vt_out[p] = total(vt_land)
    vt_all.start()

    loop(chips - 1, v_recv)
    v_out[q] = total(v_land)
    v_all.start()

    pt_cut.wait_recv()
    t_out[p] = total(t_land)
    pt_all.start()

    pc_wide.wait_recv()
    c_out[q] = total(c_row)
    c_all.start()

    v_all.relay()
    c_all.relay()
    vt_all.wait_recv()
    pt_all.wait_recv()
    v_all.finish()
    c_all.finish()

    @pl.when(first)
    def _():
        reduce.wait_send()

        @pl.when(p == 1)
        def _():
            t_cut.wait_send()

        r_cut.wait_send()
        g_down.wait_send()
        t_down.wait_send()

    @pl.when(p == 0)
    def _():
        c_cut.wait_send()

    v_swap.wait_send()
    c_swap.wait_send()
    loop(chips - 1, lambda k: v_copy(k).wait_send())
    loop(chips - 1, lambda k: c_copy(k).wait_send())
    for done in (g_wide, t_wide, c_wide, vt_cut, pt_cut, pc_wide, vt_all, pt_all):
        done.wait_send()


def main(rows, cols, band, alin, zlin):
    height = alin.shape[0] // WIDE
    count = zlin.shape[0] // WIDE
    chips, slab, piece, tp = cols // 2, height // cols, band // cols, count // rows
    dma = pltpu.SemaphoreType.DMA
    fan = [dma((rows,))] * 2
    cut = [dma((rows,)), dma]
    ring = [dma((chips,))] * 4
    half = [dma((chips,))] * 2
    vmem = pl.BlockSpec(memory_space=pltpu.VMEM)
    flat = (height, band)
    small = (rows, piece, band)
    outs = [flat, (band, height), (cols, slab, band), (rows, piece, height), (cols, piece, band), (rows, tp, band), (band, band)]
    scratch = [
        (height, height), (count, height), flat, (rows, piece, height), small, small, small, small,
        (cols, slab, band), (rows, piece, height), (band, band), (band, band),
        (2, chips, slab, band), (chips, slab, band), (chips, slab, band), (chips, slab, band),
        (rows, piece, height), (rows, piece, height),
        (2, chips, piece, band), (chips, piece, band), (chips, piece, band), (chips, piece, band), small,
        (rows, tp, band), (rows, tp, band),
    ]
    return pl.pallas_call(
        functools.partial(main_kernel, rows, cols),
        out_shape=tuple(jax.ShapeDtypeStruct(s, F32) for s in outs),
        in_specs=[vmem] * 2,
        out_specs=(vmem,) * len(outs),
        scratch_shapes=[pltpu.VMEM(s, F32) for s in scratch] + fan * 9 + cut * 5 + ring * 3 + [dma] * 4 + half * 2,
        compiler_params=pltpu.CompilerParams(collective_id=0, has_side_effects=True),
        name="main",
    )(alin, zlin)


def update_kernel(alin, zlin, y, yt, v, vt, c, t, k, a_out, z_out):
    height, band = y.shape
    count = zlin.shape[0] // WIDE
    image, image_t = v[...].reshape(height, band), vt[...].reshape(band, height)
    half = 0.5 * dot(dot(k[...], c[...].reshape(band, band), 0, 0), k[...], 1, 0)
    x = dot(image, k[...], 1, 0) - dot(y[...], half, 1, 0)
    xt = dot(k[...], image_t, 0, 0) - dot(half, yt[...], 0, 0)
    tk = dot(t[...].reshape(count, band), k[...], 1, 0)
    for lo in range(0, height, band):
        move = dot(x, yt[:, lo : lo + band], 1, 0) + dot(y[...], xt[:, lo : lo + band], 1, 0)
        turn = dot(tk, y[lo : lo + band, :], 1, 1)
        for i in range(band // 128):
            at = lo // 128 + i
            lanes = slice(128 * i, 128 * (i + 1))
            a_out[pl.ds(at, height, stride=WIDE), :] = strip_of(alin, 0, height, at) - move[:, lanes]
            z_out[pl.ds(at, count, stride=WIDE), :] = strip_of(zlin, 0, count, at) - turn[:, lanes]


def update(alin, zlin, *rest):
    vmem = pl.BlockSpec(memory_space=pltpu.VMEM)
    return pl.pallas_call(
        update_kernel,
        out_shape=(jax.ShapeDtypeStruct(alin.shape, F32), jax.ShapeDtypeStruct(zlin.shape, F32)),
        in_specs=[vmem] * (2 + len(rest)),
        out_specs=(vmem,) * 2,
        name="update",
    )(alin, zlin, *rest)


def on_device(rows, cols, matrix, vectors):
    band = matrix.shape[2]
    alin = matrix.reshape(-1, 128)
    zlin = vectors.reshape(-1, 128)
    a, z = update(alin, zlin, *main(rows, cols, band, alin, zlin))
    return a.reshape(matrix.shape), z.reshape(vectors.shape)


def solution(mesh):
    specs = (P(None, "row", None, None, "col", None), P("col", None, "row", None))
    return jax.shard_map(
        functools.partial(on_device, mesh.shape["row"], mesh.shape["col"]),
        mesh=mesh,
        in_specs=specs,
        out_specs=specs,
        check_vma=False,
    )
```

```python
import functools

import jax
import jax.numpy as jnp
from jax import lax
from jax.experimental import pallas as pl
from jax.experimental.pallas import tpu as pltpu
from jax.sharding import PartitionSpec as P

MESH = pl.DeviceIdType.MESH
F32 = jnp.float32
HIGH = lax.Precision.HIGH
HIGHEST = lax.Precision.HIGHEST
STEP = 32
GROUP = 16
WIDE = 6


def dot(a, b, ca, cb, precision=HIGH):
    return lax.dot_general(
        a, b, (((ca,), (cb,)), ((), ())), precision=precision, preferred_element_type=F32
    )


def send(src, dst, ssem, rsem, axis, to):
    return pltpu.make_async_remote_copy(
        src_ref=src, dst_ref=dst, send_sem=ssem, recv_sem=rsem, device_id={axis: to}, device_id_type=MESH
    )


def loop(n, body):
    lax.fori_loop(0, n, lambda k, c: (body(k), c)[1], 0)


def greet(rows, cols, p, q):
    barrier = pltpu.get_barrier_semaphore()

    def hello_row(k):
        pl.semaphore_signal(barrier, inc=1, device_id={"row": lax.rem(p + 1 + k, rows)}, device_id_type=MESH)

    def hello_col(k):
        pl.semaphore_signal(barrier, inc=1, device_id={"col": lax.rem(q + 1 + k, cols)}, device_id_type=MESH)

    loop(rows - 1, hello_row)
    loop(cols - 1, hello_col)
    return lambda: pl.semaphore_wait(barrier, rows + cols - 2)


class Fan:
    def __init__(self, axis, size, me, ssem, rsem, src, dst, recv=None):
        self.axis, self.size, self.me = axis, size, me
        self.ssem, self.rsem, self.src, self.dst = ssem, rsem, src, dst
        self.recv = recv

    def copy(self, k):
        to = lax.rem(self.me + 1 + k, self.size)
        return send(self.src(to), self.dst(self.me), self.ssem.at[k], self.rsem.at[self.me], self.axis, to)

    def start(self):
        loop(self.size - 1, lambda k: self.copy(k).start())

    def wait_recv(self):
        def one(k):
            at = lax.rem(self.me + 1 + k, self.size)
            ref = self.dst(at)
            send(ref, ref, self.ssem.at[k], self.rsem.at[at], self.axis, at).wait_recv()

        loop(self.size - 1, one)

    def wait_send(self):
        loop(self.size - 1, lambda k: self.copy(k).wait_send())


class Scatter:
    def __init__(self, axis, size, me, root, ssem, rsem, src, dst):
        self.axis, self.size, self.me, self.root = axis, size, me, root
        self.ssem, self.rsem, self.src, self.dst = ssem, rsem, src, dst

    def copy(self, k):
        to = lax.rem(self.me + 1 + k, self.size)
        return send(self.src(to), self.dst(to), self.ssem.at[k], self.rsem, self.axis, to)

    def start(self):
        loop(self.size - 1, lambda k: self.copy(k).start())

    def wait_recv(self):
        ref = self.dst(self.me)
        send(ref, ref, self.ssem.at[0], self.rsem, self.axis, self.root).wait_recv()

    def wait_send(self):
        loop(self.size - 1, lambda k: self.copy(k).wait_send())


class Chips:
    def __init__(self, cols, q, zs, zr, ss, sr, ref):
        self.chips, self.cols, self.q, self.ref = cols // 2, cols, q, ref
        self.z, self.c = q // 2, lax.rem(q, 2)
        self.zs, self.zr, self.ss, self.sr = zs, zr, ss, sr

    def along(self, k):
        z = lax.rem(self.z + 1 + k, self.chips)
        mine = self.ref.at[self.q]
        return send(mine, mine, self.zs.at[k], self.zr.at[self.z], "col", 2 * z + self.c)

    def across(self, z):
        piece = self.ref.at[2 * z + self.c]
        return send(piece, piece, self.ss.at[z], self.sr.at[z], "col", 2 * self.z + 1 - self.c)

    def start(self):
        loop(self.chips - 1, lambda k: self.along(k).start())
        self.across(self.z).start()

    def relay(self):
        def one(k):
            z = lax.rem(self.z + 1 + k, self.chips)
            piece = self.ref.at[2 * z + self.c]
            send(piece, piece, self.zs.at[k], self.zr.at[z], "col", 2 * z + self.c).wait_recv()
            self.across(z).start()

        loop(self.chips - 1, one)

    def finish(self):
        loop(self.chips - 1, lambda k: self.along(k).wait_send())

        def one(z):
            self.across(z).wait_send()
            piece = self.ref.at[2 * z + 1 - self.c]
            send(piece, piece, self.ss.at[z], self.sr.at[z], "col", 2 * self.z + 1 - self.c).wait_recv()

        loop(self.chips, one)


def total(ref):
    size = ref.shape[0]
    acc = ref[0]
    for i in range(1, size):
        acc = acc + ref[i]
    return acc


def splat_row(x, j):
    return jnp.broadcast_to(x[j : j + 1, :], x.shape)


def small_inverse(tile, off, chol):
    row = lax.broadcasted_iota(jnp.int32, tile.shape, 0)
    lane = lax.broadcasted_iota(jnp.int32, tile.shape, 1)
    inverse = jnp.where(row == lane, 1.0, 0.0).astype(F32)
    pivots = jnp.ones_like(tile)
    for g in range(0, STEP, GROUP):
        cols = [jnp.broadcast_to(tile[:, off + g + i : off + g + i + 1], tile.shape) for i in range(GROUP)]
        for i in range(GROUP):
            j = g + i
            pivot = splat_row(cols[i], j)
            scale = 1.0 / pivot
            if chol:
                m = jnp.where(row > j, cols[i] * scale, 0.0)
                pivots = jnp.where(row == j, pivot, pivots)
            else:
                m = jnp.where(row == j, 1.0 - scale, cols[i] * scale)
            for k in range(i + 1, GROUP):
                cols[k] = cols[k] - m * splat_row(cols[k], j)
            tile = tile - m * splat_row(tile, j)
            inverse = inverse - m * splat_row(inverse, j)
    if chol:
        inverse = inverse * lax.rsqrt(pivots)
    return inverse[:, :STEP]


def eliminate(work, out, chol, halfway=None):
    size = work.shape[0]
    lane = lax.broadcasted_iota(jnp.int32, (STEP, size), 1)
    row = lax.broadcasted_iota(jnp.int32, (STEP, size), 0)
    for at in range(0, size, STEP):
        end = at + STEP
        if halfway is not None and 2 * at == size:
            halfway()
        base = at // 128 * 128
        inverse = small_inverse(work[at:end, base : base + 128], at - base, chol)
        strip = jnp.where(
            (lane >= at) & (lane < end), jnp.where(lane - at == row, 1.0, 0.0), work[at:end, :]
        )
        strip = dot(inverse, strip, 1, 0, HIGHEST)
        if chol:
            out[at:end, :] = jnp.where(lane < end, strip, 0.0)
            spans = [(end, size)]
        else:
            spans = [(0, at), (end, size)]
        for lo, hi in spans:
            if lo == hi:
                continue
            side = work[lo:hi, at:end]
            if chol:
                side = dot(side, inverse, 1, 1, HIGHEST)
            wide = lax.broadcasted_iota(jnp.int32, (hi - lo, size), 1)
            rest = jnp.where((wide >= at) & (wide < end), 0.0, work[lo:hi, :])
            work[lo:hi, :] = rest - dot(side, strip, 1, 0, HIGHEST)
        if not chol:
            work[at:end, :] = strip


def identity(size):
    row = lax.broadcasted_iota(jnp.int32, (size, size), 0)
    return jnp.where(row == lax.broadcasted_iota(jnp.int32, (size, size), 1), 1.0, 0.0).astype(F32)


def strip_of(ref, start, count, at):
    return ref[pl.ds(start * WIDE + at, count, stride=WIDE), :]


def main_kernel(
    rows, cols, a_hbm, z_hbm,
    y_out, yt_out, v_out, vt_out, c_out, t_out, k_out,
    alin, zlin, a, z, panel, panel_t, gram, landed, g_out, top_out, rows_out, cols_out, work, w,
    v, v_half, v_sum, v_land, vt, vt_land, c, c_half, c_sum, c_land, c_row, t, t_land,
    *sems,
):
    sems = iter(sems)
    a_in = pltpu.make_async_copy(a_hbm, alin, next(sems))
    z_in = pltpu.make_async_copy(z_hbm, zlin, next(sems))
    a_in.start()
    z_in.start()
    p, q = lax.axis_index("row"), lax.axis_index("col")
    met = greet(rows, cols, p, q)
    first = q == 0
    chips = cols // 2
    my_z, core = q // 2, lax.rem(q, 2)
    other = 2 * my_z + 1 - core
    height, band = panel.shape
    slab, piece = rows_out.shape[1], top_out.shape[1]

    a_in.wait()
    row = lax.broadcasted_iota(jnp.int32, (height, 128), 0)
    for at in range(band // 128):
        panel[:, 128 * at : 128 * (at + 1)] = jnp.where((row < band) & (p == 0), 0.0, strip_of(alin, 0, height, at))
    gram[...] = dot(panel[...], panel[...], 0, 0, HIGHEST).reshape(gram.shape)
    def top_piece(to):
        return panel.at[pl.ds(pl.multiple_of(to * piece, piece), piece), :]

    def row_piece(to):
        return panel.at[pl.ds(pl.multiple_of(to * slab, slab), slab), :]

    def fan(axis, size, me, src, dst):
        return Fan(axis, size, me, next(sems), next(sems), src, dst)

    def cut(axis, size, me, root, src, dst):
        return Scatter(axis, size, me, root, next(sems), next(sems), src, dst)

    def ring(ref):
        return Chips(cols, q, next(sems), next(sems), next(sems), next(sems), ref)

    reduce = fan("row", rows, p, lambda to: gram.at[to], lambda at: landed.at[at])
    g_wide = fan("row", rows, p, lambda to: g_out.at[p], lambda at: g_out.at[at])
    t_wide = fan("row", rows, p, lambda to: top_out.at[p], lambda at: top_out.at[at])
    c_wide = fan("row", rows, p, lambda to: cols_out.at[p], lambda at: cols_out.at[at])
    vt_cut = fan("row", rows, p, lambda to: vt.at[to], lambda at: vt_land.at[at])
    pt_cut = fan("row", rows, p, lambda to: t.at[to], lambda at: t_land.at[at])
    pc_wide = fan("row", rows, p, lambda to: c_row.at[p], lambda at: c_row.at[at])
    vt_all = fan("row", rows, p, lambda to: vt_out.at[p], lambda at: vt_out.at[at])
    pt_all = fan("row", rows, p, lambda to: t_out.at[p], lambda at: t_out.at[at])
    g_down = cut("col", cols, q, 0, lambda to: g_out.at[p], lambda to: g_out.at[p])
    t_cut = cut("row", rows, p, 1, top_piece, lambda to: top_out.at[to])
    t_down = cut("col", cols, q, 0, lambda to: top_out.at[p], lambda to: top_out.at[p])
    r_cut = cut("col", cols, q, 0, row_piece, lambda to: rows_out.at[to])
    c_cut = cut("row", rows, p, 0, lambda to: panel_t.at[to], lambda to: cols_out.at[to])
    r_wide, v_all, c_all = ring(rows_out), ring(v_out), ring(c_out)

    met()

    @pl.when(first)
    def _():
        reduce.start()

        @pl.when(p == 1)
        def _():
            t_cut.start()

        r_cut.start()

    @pl.when(p == 0)
    def _():
        for at in range(WIDE):
            part = strip_of(alin, 0, band, at)
            if at < band // 128:
                part = jnp.where(q == 0, 0.0, part)
            panel_t[:, :, 128 * at : 128 * (at + 1)] = part.reshape(rows, band // rows, 128)
        c_cut.start()

    @pl.when(first)
    def _():
        landed[p] = gram[p]
        rows_out[0] = panel[:slab, :]

        @pl.when(p == 1)
        def _():
            top_out[1] = panel[piece : 2 * piece, :]

        reduce.wait_recv()
        g_out[p] = total(landed)
        g_down.start()

    @pl.when(p == 0)
    def _():
        cols_out[0] = panel_t[0]

    @pl.when(jnp.logical_not(first))
    def _():
        g_down.wait_recv()

    g_wide.start()

    @pl.when(jnp.logical_not(first))
    def _():
        r_cut.wait_recv()

    r_wide.start()

    @pl.when(p != 0)
    def _():
        c_cut.wait_recv()

    c_wide.start()

    @pl.when(first)
    def _():
        @pl.when(p != 1)
        def _():
            t_cut.wait_recv()

        t_down.start()

    @pl.when(jnp.logical_not(first))
    def _():
        t_down.wait_recv()

    t_wide.start()
    z_in.wait()
    for at in range(WIDE):
        a[:, 128 * at : 128 * (at + 1)] = strip_of(alin, 0, height, at)
        z[:, 128 * at : 128 * (at + 1)] = strip_of(zlin, 0, z.shape[0], at)
    g_wide.wait_recv()

    work[...] = g_out[...].reshape(band, band)
    eliminate(work, w, True, r_wide.relay)

    def along(src, land):
        ss, rs = next(sems), next(sems)

        def copy(k):
            to = lax.rem(my_z + 1 + k, chips)
            return send(src.at[to], land.at[my_z], ss.at[k], rs.at[my_z], "col", 2 * to + core)

        def recv(k):
            at = lax.rem(my_z + 1 + k, chips)
            send(src.at[at], land.at[at], ss.at[k], rs.at[at], "col", 2 * at + core).wait_recv()

        return copy, recv

    c_wide.wait_recv()
    yt_out[...] = dot(w[...], cols_out[...].reshape(band, height), 1, 0)

    @pl.when(q == 1)
    def _():
        yt_out[:, :band] = yt_out[:, :band] + identity(band)

    image = dot(a[...], yt_out[...], 1, 1)
    for i in range(cols):
        v[i % 2, i // 2] = image[i * slab : (i + 1) * slab, :]
    v_swap = send(v.at[1 - core], v_half, next(sems), next(sems), "col", other)
    v_swap.start()
    r_wide.finish()
    y_out[...] = dot(rows_out[...].reshape(height, band), w[...], 1, 1)

    @pl.when(p == 1)
    def _():
        y_out[:band, :] = y_out[:band, :] + identity(band)

    vt[...] = dot(y_out[...], a[...], 0, 0).reshape(vt.shape)
    vt_cut.start()
    v_swap.wait_recv()

    def v_add(i):
        v_sum[i] = v[core, i] + v_half[i]

    loop(chips, v_add)
    v_copy, v_recv = along(v_sum, v_land)
    loop(chips - 1, lambda k: v_copy(k).start())
    inner = dot(y_out[...], image, 0, 0)
    for i in range(cols):
        c[i % 2, i // 2] = inner[i * piece : (i + 1) * piece, :]
    c_swap = send(c.at[1 - core], c_half, next(sems), next(sems), "col", other)
    c_swap.start()
    t[...] = dot(z[...], y_out[...], 1, 0).reshape(t.shape)
    pt_cut.start()
    vt_land[p] = vt[p]
    t_land[p] = t[p]

    c_copy, c_recv = along(c_sum, c_land)
    c_swap.wait_recv()

    def c_add(i):
        c_sum[i] = c[core, i] + c_half[i]

    loop(chips, c_add)
    loop(chips - 1, lambda k: c_copy(k).start())
    v_land[my_z] = v_sum[my_z]
    c_land[my_z] = c_sum[my_z]

    t_wide.wait_recv()
    k_out[...] = identity(band) + dot(top_out[...].reshape(band, band), w[...], 1, 1, HIGHEST)
    eliminate(k_out, None, False)

    loop(chips - 1, c_recv)
    c_row[p] = total(c_land)
    pc_wide.start()

    vt_cut.wait_recv()
    vt_out[p] = total(vt_land)
    vt_all.start()

    loop(chips - 1, v_recv)
    v_out[q] = total(v_land)
    v_all.start()

    pt_cut.wait_recv()
    t_out[p] = total(t_land)
    pt_all.start()

    pc_wide.wait_recv()
    c_out[q] = total(c_row)
    c_all.start()

    v_all.relay()
    c_all.relay()
    vt_all.wait_recv()
    pt_all.wait_recv()
    v_all.finish()
    c_all.finish()

    @pl.when(first)
    def _():
        reduce.wait_send()

        @pl.when(p == 1)
        def _():
            t_cut.wait_send()

        r_cut.wait_send()
        g_down.wait_send()
        t_down.wait_send()

    @pl.when(p == 0)
    def _():
        c_cut.wait_send()

    v_swap.wait_send()
    c_swap.wait_send()
    loop(chips - 1, lambda k: v_copy(k).wait_send())
    loop(chips - 1, lambda k: c_copy(k).wait_send())
    for done in (g_wide, t_wide, c_wide, vt_cut, pt_cut, pc_wide, vt_all, pt_all):
        done.wait_send()


def main(rows, cols, band, alin, zlin):
    height = alin.shape[0] // WIDE
    count = zlin.shape[0] // WIDE
    chips, slab, piece, tp = cols // 2, height // cols, band // cols, count // rows
    dma = pltpu.SemaphoreType.DMA
    fan = [dma((rows,))] * 2
    cut = [dma((rows,)), dma]
    ring = [dma((chips,))] * 4
    half = [dma((chips,))] * 2
    vmem = pl.BlockSpec(memory_space=pltpu.VMEM)
    flat = (height, band)
    small = (rows, piece, band)
    outs = [flat, (band, height), (cols, slab, band), (rows, piece, height), (cols, piece, band), (rows, tp, band), (band, band)]
    scratch = [
        alin.shape, zlin.shape, (height, height), (count, height), flat, (rows, piece, height), small, small, small, small,
        (cols, slab, band), (rows, piece, height), (band, band), (band, band),
        (2, chips, slab, band), (chips, slab, band), (chips, slab, band), (chips, slab, band),
        (rows, piece, height), (rows, piece, height),
        (2, chips, piece, band), (chips, piece, band), (chips, piece, band), (chips, piece, band), small,
        (rows, tp, band), (rows, tp, band),
    ]
    return pl.pallas_call(
        functools.partial(main_kernel, rows, cols),
        out_shape=tuple(jax.ShapeDtypeStruct(s, F32) for s in outs),
        in_specs=[pl.BlockSpec(memory_space=pltpu.HBM)] * 2,
        out_specs=(vmem,) * len(outs),
        scratch_shapes=[pltpu.VMEM(s, F32) for s in scratch] + [dma] * 2 + fan * 9 + cut * 5 + ring * 3 + [dma] * 2 + half + [dma] * 2 + half,
        compiler_params=pltpu.CompilerParams(collective_id=0, has_side_effects=True, vmem_limit_bytes=50 * 2**20),
        name="main",
    )(alin, zlin)


def update_kernel(alin, zlin, y, yt, v, vt, c, t, k, a_out, z_out):
    height, band = y.shape
    count = zlin.shape[0] // WIDE
    image, image_t = v[...].reshape(height, band), vt[...].reshape(band, height)
    half = 0.5 * dot(dot(k[...], c[...].reshape(band, band), 0, 0), k[...], 1, 0)
    x = dot(image, k[...], 1, 0) - dot(y[...], half, 1, 0)
    xt = dot(k[...], image_t, 0, 0) - dot(half, yt[...], 0, 0)
    tk = dot(t[...].reshape(count, band), k[...], 1, 0)
    for lo in range(0, height, band):
        move = dot(x, yt[:, lo : lo + band], 1, 0) + dot(y[...], xt[:, lo : lo + band], 1, 0)
        turn = dot(tk, y[lo : lo + band, :], 1, 1)
        for i in range(band // 128):
            at = lo // 128 + i
            lanes = slice(128 * i, 128 * (i + 1))
            a_out[pl.ds(at, height, stride=WIDE), :] = strip_of(alin, 0, height, at) - move[:, lanes]
            z_out[pl.ds(at, count, stride=WIDE), :] = strip_of(zlin, 0, count, at) - turn[:, lanes]


def update(alin, zlin, *rest):
    vmem = pl.BlockSpec(memory_space=pltpu.VMEM)
    return pl.pallas_call(
        update_kernel,
        out_shape=(jax.ShapeDtypeStruct(alin.shape, F32), jax.ShapeDtypeStruct(zlin.shape, F32)),
        in_specs=[vmem] * (2 + len(rest)),
        out_specs=(vmem,) * 2,
        compiler_params=pltpu.CompilerParams(vmem_limit_bytes=24 * 2**20),
        name="update",
    )(alin, zlin, *rest)


def on_device(rows, cols, matrix, vectors):
    band = matrix.shape[2]
    alin = matrix.reshape(-1, 128)
    zlin = vectors.reshape(-1, 128)
    a, z = update(alin, zlin, *main(rows, cols, band, alin, zlin))
    return a.reshape(matrix.shape), z.reshape(vectors.shape)


def solution(mesh):
    specs = (P(None, "row", None, None, "col", None), P("col", None, "row", None))
    return jax.shard_map(
        functools.partial(on_device, mesh.shape["row"], mesh.shape["col"]),
        mesh=mesh,
        in_specs=specs,
        out_specs=specs,
        check_vma=False,
    )
```

```python
import functools

import jax
import jax.numpy as jnp
from jax import lax
from jax.experimental import pallas as pl
from jax.experimental.pallas import tpu as pltpu
from jax.sharding import PartitionSpec as P

MESH = pl.DeviceIdType.MESH
F32 = jnp.float32
HIGH = lax.Precision.HIGH
HIGHEST = lax.Precision.HIGHEST
STEP = 64
GROUP = 16
WIDE = 6


def dot(a, b, ca, cb, precision=HIGH):
    return lax.dot_general(
        a, b, (((ca,), (cb,)), ((), ())), precision=precision, preferred_element_type=F32
    )


def send(src, dst, ssem, rsem, axis, to):
    return pltpu.make_async_remote_copy(
        src_ref=src, dst_ref=dst, send_sem=ssem, recv_sem=rsem, device_id={axis: to}, device_id_type=MESH
    )


def loop(n, body):
    lax.fori_loop(0, n, lambda k, c: (body(k), c)[1], 0)


def greet(rows, cols, p, q):
    barrier = pltpu.get_barrier_semaphore()

    def hello_row(k):
        pl.semaphore_signal(barrier, inc=1, device_id={"row": lax.rem(p + 1 + k, rows)}, device_id_type=MESH)

    def hello_col(k):
        pl.semaphore_signal(barrier, inc=1, device_id={"col": lax.rem(q + 1 + k, cols)}, device_id_type=MESH)

    loop(rows - 1, hello_row)
    loop(cols - 1, hello_col)
    return lambda: pl.semaphore_wait(barrier, rows + cols - 2)


class Fan:
    def __init__(self, axis, size, me, ssem, rsem, src, dst, recv=None):
        self.axis, self.size, self.me = axis, size, me
        self.ssem, self.rsem, self.src, self.dst = ssem, rsem, src, dst
        self.recv = recv

    def copy(self, k):
        to = lax.rem(self.me + 1 + k, self.size)
        return send(self.src(to), self.dst(self.me), self.ssem.at[k], self.rsem.at[self.me], self.axis, to)

    def start(self):
        loop(self.size - 1, lambda k: self.copy(k).start())

    def wait_recv(self):
        def one(k):
            at = lax.rem(self.me + 1 + k, self.size)
            ref = self.dst(at)
            send(ref, ref, self.ssem.at[k], self.rsem.at[at], self.axis, at).wait_recv()

        loop(self.size - 1, one)

    def wait_send(self):
        loop(self.size - 1, lambda k: self.copy(k).wait_send())


class Scatter:
    def __init__(self, axis, size, me, root, ssem, rsem, src, dst):
        self.axis, self.size, self.me, self.root = axis, size, me, root
        self.ssem, self.rsem, self.src, self.dst = ssem, rsem, src, dst

    def copy(self, k):
        to = lax.rem(self.me + 1 + k, self.size)
        return send(self.src(to), self.dst(to), self.ssem.at[k], self.rsem, self.axis, to)

    def start(self):
        loop(self.size - 1, lambda k: self.copy(k).start())

    def wait_recv(self):
        ref = self.dst(self.me)
        send(ref, ref, self.ssem.at[0], self.rsem, self.axis, self.root).wait_recv()

    def wait_send(self):
        loop(self.size - 1, lambda k: self.copy(k).wait_send())


class Chips:
    def __init__(self, cols, q, zs, zr, ss, sr, at):
        self.chips, self.cols, self.q, self.at = cols // 2, cols, q, at
        self.z, self.c = q // 2, lax.rem(q, 2)
        self.zs, self.zr, self.ss, self.sr = zs, zr, ss, sr

    def along(self, k):
        z = lax.rem(self.z + 1 + k, self.chips)
        mine = self.at(self.q)
        return send(mine, mine, self.zs.at[k], self.zr.at[self.z], "col", 2 * z + self.c)

    def across(self, z):
        piece = self.at(2 * z + self.c)
        return send(piece, piece, self.ss.at[z], self.sr.at[z], "col", 2 * self.z + 1 - self.c)

    def start(self):
        loop(self.chips - 1, lambda k: self.along(k).start())
        self.across(self.z).start()

    def relay(self):
        def one(k):
            z = lax.rem(self.z + 1 + k, self.chips)
            piece = self.at(2 * z + self.c)
            send(piece, piece, self.zs.at[k], self.zr.at[z], "col", 2 * z + self.c).wait_recv()
            self.across(z).start()

        loop(self.chips - 1, one)

    def finish(self):
        loop(self.chips - 1, lambda k: self.along(k).wait_send())

        def one(z):
            self.across(z).wait_send()
            piece = self.at(2 * z + 1 - self.c)
            send(piece, piece, self.ss.at[z], self.sr.at[z], "col", 2 * self.z + 1 - self.c).wait_recv()

        loop(self.chips, one)


def total(ref):
    size = ref.shape[0]
    acc = ref[0]
    for i in range(1, size):
        acc = acc + ref[i]
    return acc


def splat_row(x, j):
    return jnp.broadcast_to(x[j : j + 1, :], x.shape)


def small_factor(tile, off):
    row = lax.broadcasted_iota(jnp.int32, tile.shape, 0)
    lane = lax.broadcasted_iota(jnp.int32, tile.shape, 1)
    inverse = jnp.where(row == lane, 1.0, 0.0).astype(F32)
    done, pivots = [], []
    for g in range(0, STEP, GROUP):
        cols = [jnp.broadcast_to(tile[:, off + g + i : off + g + i + 1], tile.shape) for i in range(GROUP)]
        row = lax.broadcasted_iota(jnp.int32, tile.shape, 0)
        for i in range(0, GROUP, 2):
            here, there = cols[i], cols[i + 1]
            a, b, d = splat_row(here, i), splat_row(there, i), splat_row(there, i + 1)
            det = a * d - b * b
            over_a, over_det = 1.0 / a, 1.0 / det
            pivots += [a[:1, :], (det * over_a)[:1, :]]
            m0 = jnp.where(row > i + 1, (here * d - there * b) * over_det, jnp.where(row == i + 1, b * over_a, 0.0))
            m1 = jnp.where(row > i + 1, (there * a - here * b) * over_det, 0.0)
            for k in range(i + 2, GROUP):
                cols[k] = cols[k] - m0 * splat_row(cols[k], i) - m1 * splat_row(cols[k], i + 1)
            if g + GROUP < STEP:
                tile = tile - m0 * splat_row(tile, i) - m1 * splat_row(tile, i + 1)
            inverse = inverse - m0 * splat_row(inverse, i) - m1 * splat_row(inverse, i + 1)
        done.append(inverse[:GROUP, :])
        tile, inverse = tile[GROUP:, :], inverse[GROUP:, :]
    inverse = jnp.concatenate(done, axis=0) * lax.rsqrt(jnp.concatenate(pivots, axis=0))
    return inverse[:, :STEP]


def small_inverse(tile, off):
    row = lax.broadcasted_iota(jnp.int32, tile.shape, 0)
    lane = lax.broadcasted_iota(jnp.int32, tile.shape, 1)
    inverse = jnp.where(row == lane, 1.0, 0.0).astype(F32)
    for g in range(0, STEP, GROUP):
        cols = [jnp.broadcast_to(tile[:, off + g + i : off + g + i + 1], tile.shape) for i in range(GROUP)]
        for i in range(GROUP):
            j = g + i
            scale = 1.0 / splat_row(cols[i], j)
            m = jnp.where(row == j, 1.0 - scale, cols[i] * scale)
            for k in range(i + 1, GROUP):
                cols[k] = cols[k] - m * splat_row(cols[k], j)
            tile = tile - m * splat_row(tile, j)
            inverse = inverse - m * splat_row(inverse, j)
    return inverse[:, :STEP]


def cholesky_inverse(gram, work, out, halfway=None):
    size = gram.shape[0]
    diagonal = jnp.where(identity(size) > 0.0, gram, 0.0)
    across = lax.rsqrt(jnp.sum(diagonal, axis=0, keepdims=True))
    work[...] = gram * across * lax.rsqrt(jnp.sum(diagonal, axis=1, keepdims=True))
    eliminate(work, out, True, halfway)
    out[...] = out[...] * across


def eliminate(work, out, chol, halfway=None):
    size = work.shape[0]
    lane = lax.broadcasted_iota(jnp.int32, (STEP, size), 1)
    row = lax.broadcasted_iota(jnp.int32, (STEP, size), 0)
    for at in range(0, size, STEP):
        end = at + STEP
        if halfway is not None and 2 * at == size:
            halfway()
        base = at // 128 * 128
        tile = work[at:end, base : base + 128]
        inverse = small_factor(tile, at - base) if chol else small_inverse(tile, at - base)
        strip = jnp.where(
            (lane >= at) & (lane < end), jnp.where(lane - at == row, 1.0, 0.0), work[at:end, :]
        )
        strip = dot(inverse, strip, 1, 0, HIGHEST)
        if chol:
            out[at:end, :] = jnp.where(lane < end, strip, 0.0)
            spans = [(end, size)]
        else:
            spans = [(0, at), (end, size)]
        for lo, hi in spans:
            if lo == hi:
                continue
            side = work[lo:hi, at:end]
            if chol:
                side = dot(side, inverse, 1, 1, HIGHEST)
            wide = lax.broadcasted_iota(jnp.int32, (hi - lo, size), 1)
            rest = jnp.where((wide >= at) & (wide < end), 0.0, work[lo:hi, :])
            work[lo:hi, :] = rest - dot(side, strip, 1, 0, HIGHEST)
        if not chol:
            work[at:end, :] = strip


def identity(size):
    row = lax.broadcasted_iota(jnp.int32, (size, size), 0)
    return jnp.where(row == lax.broadcasted_iota(jnp.int32, (size, size), 1), 1.0, 0.0).astype(F32)


def strip_of(ref, start, count, at):
    return ref[pl.ds(start * WIDE + at, count, stride=WIDE), :]


def main_kernel(
    rows, cols, a_hbm, z_hbm,
    y_out, yt_out, x_out, xt_out, tk_out,
    v_out, vt_out, c_out, t_out, k_out, alin, zlin, a, z, panel, panel_t, gram, landed, g_out, top_out, rows_out, cols_out, work, w,
    v, v_half, v_sum, v_land, vt, vt_land, c, c_half, c_sum, c_land, c_row, t, t_land,
    *sems,
):
    sems = iter(sems)
    a_in = pltpu.make_async_copy(a_hbm, alin, next(sems))
    z_in = pltpu.make_async_copy(z_hbm, zlin, next(sems))
    a_in.start()
    z_in.start()
    p, q = lax.axis_index("row"), lax.axis_index("col")
    met = greet(rows, cols, p, q)
    first = q == 0
    chips = cols // 2
    my_z, core = q // 2, lax.rem(q, 2)
    other = 2 * my_z + 1 - core
    height, band = panel.shape
    slab, piece = rows_out.shape[1], top_out.shape[1]

    a_in.wait()
    row = lax.broadcasted_iota(jnp.int32, (height, 128), 0)
    for at in range(band // 128):
        panel[:, 128 * at : 128 * (at + 1)] = jnp.where((row < band) & (p == 0), 0.0, strip_of(alin, 0, height, at))
    gram[...] = dot(panel[...], panel[...], 0, 0, HIGHEST).reshape(gram.shape)
    def top_piece(to):
        return panel.at[pl.ds(pl.multiple_of(to * piece, piece), piece), :]

    def row_piece(to):
        return panel.at[pl.ds(pl.multiple_of(to * slab, slab), slab), :]

    def fan(axis, size, me, src, dst):
        return Fan(axis, size, me, next(sems), next(sems), src, dst)

    def cut(axis, size, me, root, src, dst):
        return Scatter(axis, size, me, root, next(sems), next(sems), src, dst)

    def ring(at):
        return Chips(cols, q, next(sems), next(sems), next(sems), next(sems), at)

    tall, flat = slab // 2, piece // 2
    halves = [(pl.ds(0, tall), pl.ds(0, flat)), (pl.ds(tall, tall), pl.ds(flat, flat))]

    reduce = fan("row", rows, p, lambda to: gram.at[to], lambda at: landed.at[at])
    g_wide = fan("row", rows, p, lambda to: g_out.at[p], lambda at: g_out.at[at])
    t_wide = fan("row", rows, p, lambda to: top_out.at[p], lambda at: top_out.at[at])
    c_wide = fan("row", rows, p, lambda to: cols_out.at[p], lambda at: cols_out.at[at])
    vt_cut = [
        fan("row", rows, p, lambda to, part=part: vt.at[to, part], lambda at, part=part: vt_land.at[at, part])
        for _, part in halves
    ]
    pt_cut = fan("row", rows, p, lambda to: t.at[to], lambda at: t_land.at[at])
    pc_wide = fan("row", rows, p, lambda to: c_row.at[p], lambda at: c_row.at[at])
    vt_all = [
        fan("row", rows, p, lambda to, part=part: vt_out.at[p, part], lambda at, part=part: vt_out.at[at, part])
        for _, part in halves
    ]
    pt_all = fan("row", rows, p, lambda to: t_out.at[p], lambda at: t_out.at[at])
    g_down = cut("col", cols, q, 0, lambda to: g_out.at[p], lambda to: g_out.at[p])
    t_cut = cut("row", rows, p, 1, top_piece, lambda to: top_out.at[to])
    t_down = cut("col", cols, q, 0, lambda to: top_out.at[p], lambda to: top_out.at[p])
    r_cut = cut("col", cols, q, 0, row_piece, lambda to: rows_out.at[to])
    c_cut = cut("row", rows, p, 0, lambda to: panel_t.at[to], lambda to: cols_out.at[to])
    r_wide, c_all = ring(lambda i: rows_out.at[i]), ring(lambda i: c_out.at[i])
    v_all = [ring(lambda i, part=part: v_out.at[i, part]) for part, _ in halves]

    met()

    @pl.when(first)
    def _():
        reduce.start()

        @pl.when(p == 1)
        def _():
            t_cut.start()

        r_cut.start()

    @pl.when(p == 0)
    def _():
        for at in range(WIDE):
            part = strip_of(alin, 0, band, at)
            if at < band // 128:
                part = jnp.where(q == 0, 0.0, part)
            panel_t[:, :, 128 * at : 128 * (at + 1)] = part.reshape(rows, band // rows, 128)
        c_cut.start()

    @pl.when(first)
    def _():
        landed[p] = gram[p]
        rows_out[0] = panel[:slab, :]

        @pl.when(p == 1)
        def _():
            top_out[1] = panel[piece : 2 * piece, :]

        reduce.wait_recv()
        g_out[p] = total(landed)
        g_down.start()

    @pl.when(p == 0)
    def _():
        cols_out[0] = panel_t[0]

    @pl.when(jnp.logical_not(first))
    def _():
        g_down.wait_recv()

    g_wide.start()

    @pl.when(jnp.logical_not(first))
    def _():
        r_cut.wait_recv()

    r_wide.start()

    @pl.when(p != 0)
    def _():
        c_cut.wait_recv()

    c_wide.start()

    @pl.when(first)
    def _():
        @pl.when(p != 1)
        def _():
            t_cut.wait_recv()

        t_down.start()

    @pl.when(jnp.logical_not(first))
    def _():
        t_down.wait_recv()

    t_wide.start()
    z_in.wait()
    for at in range(WIDE):
        a[:, 128 * at : 128 * (at + 1)] = strip_of(alin, 0, height, at)
        z[:, 128 * at : 128 * (at + 1)] = strip_of(zlin, 0, z.shape[0], at)
    g_wide.wait_recv()

    cholesky_inverse(g_out[...].reshape(band, band), work, w, r_wide.relay)

    def along(src, land, part):
        ss, rs = next(sems), next(sems)

        def copy(k):
            to = lax.rem(my_z + 1 + k, chips)
            return send(src.at[to, part], land.at[my_z, part], ss.at[k], rs.at[my_z], "col", 2 * to + core)

        def recv(k):
            at = lax.rem(my_z + 1 + k, chips)
            send(src.at[at, part], land.at[at, part], ss.at[k], rs.at[at], "col", 2 * at + core).wait_recv()

        return copy, recv

    c_wide.wait_recv()
    yt_out[...] = dot(w[...], cols_out[...].reshape(band, height), 1, 0)

    @pl.when(q == 1)
    def _():
        yt_out[:, :band] = yt_out[:, :band] + identity(band)

    image = dot(a[...], yt_out[...], 1, 1)
    for i in range(cols):
        v[i % 2, i // 2] = image[i * slab : (i + 1) * slab, :]
    v_swap = send(v.at[1 - core], v_half, next(sems), next(sems), "col", other)
    v_swap.start()
    r_wide.finish()
    y_out[...] = dot(rows_out[...].reshape(height, band), w[...], 1, 1)

    @pl.when(p == 1)
    def _():
        y_out[:band, :] = y_out[:band, :] + identity(band)

    vt[...] = dot(y_out[...], a[...], 0, 0).reshape(vt.shape)
    vt_cut[0].start()
    vt_cut[1].start()
    v_swap.wait_recv()

    def v_add(i):
        v_sum[i] = v[core, i] + v_half[i]

    loop(chips, v_add)
    v_along = [along(v_sum, v_land, part) for part, _ in halves]
    for copy, _ in v_along:
        loop(chips - 1, lambda k, copy=copy: copy(k).start())
    inner = dot(y_out[...], image, 0, 0)
    for i in range(cols):
        c[i % 2, i // 2] = inner[i * piece : (i + 1) * piece, :]
    c_swap = send(c.at[1 - core], c_half, next(sems), next(sems), "col", other)
    c_swap.start()
    t[...] = dot(z[...], y_out[...], 1, 0).reshape(t.shape)
    pt_cut.start()
    vt_land[p] = vt[p]
    t_land[p] = t[p]

    c_copy, c_recv = along(c_sum, c_land, pl.ds(0, piece))
    c_swap.wait_recv()

    def c_add(i):
        c_sum[i] = c[core, i] + c_half[i]

    loop(chips, c_add)
    loop(chips - 1, lambda k: c_copy(k).start())
    v_land[my_z] = v_sum[my_z]
    c_land[my_z] = c_sum[my_z]

    t_wide.wait_recv()
    k_out[...] = identity(band) + dot(top_out[...].reshape(band, band), w[...], 1, 1, HIGHEST)
    def send_on(n):
        tall_part, flat_part = halves[n]
        loop(chips - 1, v_along[n][1])
        v_out[q, tall_part] = total(v_land.at[:, tall_part])
        v_all[n].start()
        vt_cut[n].wait_recv()
        vt_out[p, flat_part] = total(vt_land.at[:, flat_part])
        vt_all[n].start()

    eliminate(k_out, None, False, lambda: send_on(0))
    loop(chips - 1, c_recv)
    c_row[p] = total(c_land)
    pc_wide.start()
    send_on(1)
    pt_cut.wait_recv()
    t_out[p] = total(t_land)
    pt_all.start()
    v_all[0].relay()
    pc_wide.wait_recv()
    c_out[q] = total(c_row)
    c_all.start()
    v_all[1].relay()
    c_all.relay()

    vt_all[0].wait_recv()
    vt_all[1].wait_recv()
    c_all.finish()
    inner_half = 0.5 * dot(dot(k_out[...], c_out[...].reshape(band, band), 0, 0), k_out[...], 1, 0)
    xt_out[...] = dot(k_out[...], vt_out[...].reshape(band, height), 0, 0) - dot(inner_half, yt_out[...], 0, 0)
    x_out[...] = dot(y_out[...], inner_half, 1, 0)
    pt_all.wait_recv()
    tk_out[...] = dot(t_out[...].reshape(tk_out.shape), k_out[...], 1, 0)
    v_all[0].finish()
    v_all[1].finish()
    x_out[...] = dot(v_out[...].reshape(height, band), k_out[...], 1, 0) - x_out[...]

    @pl.when(first)
    def _():
        reduce.wait_send()

        @pl.when(p == 1)
        def _():
            t_cut.wait_send()

        r_cut.wait_send()
        g_down.wait_send()
        t_down.wait_send()

    @pl.when(p == 0)
    def _():
        c_cut.wait_send()

    v_swap.wait_send()
    c_swap.wait_send()
    for copy, _ in v_along:
        loop(chips - 1, lambda k, copy=copy: copy(k).wait_send())
    loop(chips - 1, lambda k: c_copy(k).wait_send())
    for done in (g_wide, t_wide, c_wide, *vt_cut, pt_cut, pc_wide, *vt_all, pt_all):
        done.wait_send()


def main(rows, cols, band, alin, zlin):
    height = alin.shape[0] // WIDE
    count = zlin.shape[0] // WIDE
    chips, slab, piece, tp = cols // 2, height // cols, band // cols, count // rows
    dma = pltpu.SemaphoreType.DMA
    fan = [dma((rows,))] * 2
    cut = [dma((rows,)), dma]
    ring = [dma((chips,))] * 4
    half = [dma((chips,))] * 2
    vmem = pl.BlockSpec(memory_space=pltpu.VMEM)
    flat = (height, band)
    small = (rows, piece, band)
    outs = [flat, (band, height), flat, (band, height), (count, band)]
    scratch = [
        (cols, slab, band), (rows, piece, height), (cols, piece, band), (rows, tp, band), (band, band), alin.shape, zlin.shape, (height, height), (count, height), flat, (rows, piece, height), small, small, small, small,
        (cols, slab, band), (rows, piece, height), (band, band), (band, band),
        (2, chips, slab, band), (chips, slab, band), (chips, slab, band), (chips, slab, band),
        (rows, piece, height), (rows, piece, height),
        (2, chips, piece, band), (chips, piece, band), (chips, piece, band), (chips, piece, band), small,
        (rows, tp, band), (rows, tp, band),
    ]
    return pl.pallas_call(
        functools.partial(main_kernel, rows, cols),
        out_shape=tuple(jax.ShapeDtypeStruct(s, F32) for s in outs),
        in_specs=[pl.BlockSpec(memory_space=pltpu.HBM)] * 2,
        out_specs=(vmem,) * len(outs),
        scratch_shapes=[pltpu.VMEM(s, F32) for s in scratch] + [dma] * 2 + fan * 11 + cut * 5 + ring * 4 + [dma] * 2 + half * 2 + [dma] * 2 + half,
        compiler_params=pltpu.CompilerParams(collective_id=0, has_side_effects=True, vmem_limit_bytes=50 * 2**20),
        name="main",
    )(alin, zlin)


def update_kernel(alin, zlin, y, yt, x, xt, tk, a_hbm, z_hbm, a_out, z_out, sems):
    height, band = y.shape
    count = zlin.shape[0] // WIDE
    copies = []

    def put(src, dst, lines, n):
        copies.append(pltpu.make_async_copy(src.at[lines, :], dst.at[lines, :], sems.at[n]))
        copies[-1].start()

    parts = height // band
    for n in range(parts):
        lo = n * band
        block = slice(lo, lo + band)
        move = dot(x[block, :], yt[...], 1, 0) + dot(y[block, :], xt[...], 1, 0)
        for at in range(WIDE):
            lines = pl.ds(lo * WIDE + at, band, stride=WIDE)
            a_out[lines, :] = alin[lines, :] - move[:, 128 * at : 128 * (at + 1)]
        put(a_out, a_hbm, pl.ds(lo * WIDE, band * WIDE), n)
    turn = dot(tk[...], y[...], 1, 1)
    for at in range(WIDE):
        lines = pl.ds(at, count, stride=WIDE)
        z_out[lines, :] = zlin[lines, :] - turn[:, 128 * at : 128 * (at + 1)]
    put(z_out, z_hbm, pl.ds(0, count * WIDE), parts)
    for copy in copies:
        copy.wait()


def update(alin, zlin, *rest):
    vmem = pl.BlockSpec(memory_space=pltpu.VMEM)
    height, band = rest[0].shape
    return pl.pallas_call(
        update_kernel,
        out_shape=(jax.ShapeDtypeStruct(alin.shape, F32), jax.ShapeDtypeStruct(zlin.shape, F32)),
        in_specs=[vmem] * (2 + len(rest)),
        out_specs=(pl.BlockSpec(memory_space=pltpu.HBM),) * 2,
        scratch_shapes=[
            pltpu.VMEM(alin.shape, F32),
            pltpu.VMEM(zlin.shape, F32),
            pltpu.SemaphoreType.DMA((height // band + 1,)),
        ],
        compiler_params=pltpu.CompilerParams(vmem_limit_bytes=24 * 2**20),
        name="update",
    )(alin, zlin, *rest)


def on_device(rows, cols, matrix, vectors):
    band = matrix.shape[2]
    alin = matrix.reshape(-1, 128)
    zlin = vectors.reshape(-1, 128)
    a, z = update(alin, zlin, *main(rows, cols, band, alin, zlin))
    return a.reshape(matrix.shape), z.reshape(vectors.shape)


def solution(mesh):
    specs = (P(None, "row", None, None, "col", None), P("col", None, "row", None))
    return jax.shard_map(
        functools.partial(on_device, mesh.shape["row"], mesh.shape["col"]),
        mesh=mesh,
        in_specs=specs,
        out_specs=specs,
        check_vma=False,
    )
```

```python
import functools

import jax
import jax.numpy as jnp
from jax import lax
from jax.experimental import pallas as pl
from jax.experimental.pallas import tpu as pltpu
from jax.sharding import PartitionSpec as P

MESH = pl.DeviceIdType.MESH
F32 = jnp.float32
HIGH = lax.Precision.HIGH
HIGHEST = lax.Precision.HIGHEST
STEP = 64
FINE = 32
GROUP = 16
WIDE = 6


def dot(a, b, ca, cb, precision=HIGH):
    return lax.dot_general(
        a, b, (((ca,), (cb,)), ((), ())), precision=precision, preferred_element_type=F32
    )


def send(src, dst, ssem, rsem, axis, to):
    return pltpu.make_async_remote_copy(
        src_ref=src, dst_ref=dst, send_sem=ssem, recv_sem=rsem, device_id={axis: to}, device_id_type=MESH
    )


def loop(n, body):
    lax.fori_loop(0, n, lambda k, c: (body(k), c)[1], 0)


def greet(rows, cols, p, q):
    barrier = pltpu.get_barrier_semaphore()

    def hello_row(k):
        pl.semaphore_signal(barrier, inc=1, device_id={"row": lax.rem(p + 1 + k, rows)}, device_id_type=MESH)

    def hello_col(k):
        pl.semaphore_signal(barrier, inc=1, device_id={"col": lax.rem(q + 1 + k, cols)}, device_id_type=MESH)

    loop(rows - 1, hello_row)
    loop(cols - 1, hello_col)
    return lambda: pl.semaphore_wait(barrier, rows + cols - 2)


class Fan:
    def __init__(self, axis, size, me, ssem, rsem, src, dst, recv=None):
        self.axis, self.size, self.me = axis, size, me
        self.ssem, self.rsem, self.src, self.dst = ssem, rsem, src, dst
        self.recv = recv

    def copy(self, k):
        to = lax.rem(self.me + 1 + k, self.size)
        return send(self.src(to), self.dst(self.me), self.ssem.at[k], self.rsem.at[self.me], self.axis, to)

    def start(self):
        loop(self.size - 1, lambda k: self.copy(k).start())

    def wait_recv(self):
        def one(k):
            at = lax.rem(self.me + 1 + k, self.size)
            ref = self.dst(at)
            send(ref, ref, self.ssem.at[k], self.rsem.at[at], self.axis, at).wait_recv()

        loop(self.size - 1, one)

    def wait_send(self):
        loop(self.size - 1, lambda k: self.copy(k).wait_send())


class Scatter:
    def __init__(self, axis, size, me, root, ssem, rsem, src, dst):
        self.axis, self.size, self.me, self.root = axis, size, me, root
        self.ssem, self.rsem, self.src, self.dst = ssem, rsem, src, dst

    def copy(self, k):
        to = lax.rem(self.me + 1 + k, self.size)
        return send(self.src(to), self.dst(to), self.ssem.at[k], self.rsem, self.axis, to)

    def start(self):
        loop(self.size - 1, lambda k: self.copy(k).start())

    def wait_recv(self):
        ref = self.dst(self.me)
        send(ref, ref, self.ssem.at[0], self.rsem, self.axis, self.root).wait_recv()

    def wait_send(self):
        loop(self.size - 1, lambda k: self.copy(k).wait_send())


class Chips:
    def __init__(self, cols, q, zs, zr, ss, sr, at):
        self.chips, self.cols, self.q, self.at = cols // 2, cols, q, at
        self.z, self.c = q // 2, lax.rem(q, 2)
        self.zs, self.zr, self.ss, self.sr = zs, zr, ss, sr

    def along(self, k):
        z = lax.rem(self.z + 1 + k, self.chips)
        mine = self.at(self.q)
        return send(mine, mine, self.zs.at[k], self.zr.at[self.z], "col", 2 * z + self.c)

    def across(self, z):
        piece = self.at(2 * z + self.c)
        return send(piece, piece, self.ss.at[z], self.sr.at[z], "col", 2 * self.z + 1 - self.c)

    def start(self):
        loop(self.chips - 1, lambda k: self.along(k).start())
        self.across(self.z).start()

    def relay(self):
        def one(k):
            z = lax.rem(self.z + 1 + k, self.chips)
            piece = self.at(2 * z + self.c)
            send(piece, piece, self.zs.at[k], self.zr.at[z], "col", 2 * z + self.c).wait_recv()
            self.across(z).start()

        loop(self.chips - 1, one)

    def finish(self):
        loop(self.chips - 1, lambda k: self.along(k).wait_send())

        def one(z):
            self.across(z).wait_send()
            piece = self.at(2 * z + 1 - self.c)
            send(piece, piece, self.ss.at[z], self.sr.at[z], "col", 2 * self.z + 1 - self.c).wait_recv()

        loop(self.chips, one)


def total(ref):
    size = ref.shape[0]
    acc = ref[0]
    for i in range(1, size):
        acc = acc + ref[i]
    return acc


def splat_row(x, j):
    return jnp.broadcast_to(x[j : j + 1, :], x.shape)


def small_factor(tile, off):
    row = lax.broadcasted_iota(jnp.int32, tile.shape, 0)
    lane = lax.broadcasted_iota(jnp.int32, tile.shape, 1)
    inverse = jnp.where(row == lane, 1.0, 0.0).astype(F32)
    done, pivots = [], []
    for g in range(0, STEP, GROUP):
        cols = [jnp.broadcast_to(tile[:, off + g + i : off + g + i + 1], tile.shape) for i in range(GROUP)]
        row = lax.broadcasted_iota(jnp.int32, tile.shape, 0)
        for i in range(0, GROUP, 2):
            here, there = cols[i], cols[i + 1]
            a, b, d = splat_row(here, i), splat_row(there, i), splat_row(there, i + 1)
            det = a * d - b * b
            over_a, over_det = 1.0 / a, 1.0 / det
            pivots += [a[:1, :], (det * over_a)[:1, :]]
            m0 = jnp.where(row > i + 1, (here * d - there * b) * over_det, jnp.where(row == i + 1, b * over_a, 0.0))
            m1 = jnp.where(row > i + 1, (there * a - here * b) * over_det, 0.0)
            for k in range(i + 2, GROUP):
                cols[k] = cols[k] - m0 * splat_row(cols[k], i) - m1 * splat_row(cols[k], i + 1)
            if g + GROUP < STEP:
                tile = tile - m0 * splat_row(tile, i) - m1 * splat_row(tile, i + 1)
            inverse = inverse - m0 * splat_row(inverse, i) - m1 * splat_row(inverse, i + 1)
        done.append(inverse[:GROUP, :])
        tile, inverse = tile[GROUP:, :], inverse[GROUP:, :]
    inverse = jnp.concatenate(done, axis=0) * lax.rsqrt(jnp.concatenate(pivots, axis=0))
    return inverse[:, :STEP]


def small_inverse(tile, off):
    row = lax.broadcasted_iota(jnp.int32, tile.shape, 0)
    lane = lax.broadcasted_iota(jnp.int32, tile.shape, 1)
    inverse = jnp.where(row == lane, 1.0, 0.0).astype(F32)
    for g in range(0, FINE, GROUP):
        cols = [jnp.broadcast_to(tile[:, off + g + i : off + g + i + 1], tile.shape) for i in range(GROUP)]
        for i in range(GROUP):
            j = g + i
            scale = 1.0 / splat_row(cols[i], j)
            m = jnp.where(row == j, 1.0 - scale, cols[i] * scale)
            for k in range(i + 1, GROUP):
                cols[k] = cols[k] - m * splat_row(cols[k], j)
            tile = tile - m * splat_row(tile, j)
            inverse = inverse - m * splat_row(inverse, j)
    return inverse[:, :FINE]


def cholesky_inverse(gram, work, out):
    size = gram.shape[0]
    diagonal = jnp.where(identity(size) > 0.0, gram, 0.0)
    across = lax.rsqrt(jnp.sum(diagonal, axis=0, keepdims=True))
    work[...] = gram * across * lax.rsqrt(jnp.sum(diagonal, axis=1, keepdims=True))
    eliminate(work, out, True)
    out[...] = out[...] * across


def eliminate(work, out, chol, between=()):
    size = work.shape[0]
    step = STEP if chol else FINE
    lane = lax.broadcasted_iota(jnp.int32, (step, size), 1)
    row = lax.broadcasted_iota(jnp.int32, (step, size), 0)
    for at in range(0, size, step):
        end = at + step
        for when, act in between:
            if when == at // step:
                act()
        base = at // 128 * 128
        tile = work[at:end, base : base + 128]
        inverse = small_factor(tile, at - base) if chol else small_inverse(tile, at - base)
        strip = jnp.where(
            (lane >= at) & (lane < end), jnp.where(lane - at == row, 1.0, 0.0), work[at:end, :]
        )
        strip = dot(inverse, strip, 1, 0, HIGHEST)
        if chol:
            out[at:end, :] = jnp.where(lane < end, strip, 0.0)
            spans = [(end, size)]
        else:
            spans = [(0, at), (end, size)]
        for lo, hi in spans:
            if lo == hi:
                continue
            side = work[lo:hi, at:end]
            if chol:
                side = dot(side, inverse, 1, 1, HIGHEST)
            wide = lax.broadcasted_iota(jnp.int32, (hi - lo, size), 1)
            rest = jnp.where((wide >= at) & (wide < end), 0.0, work[lo:hi, :])
            work[lo:hi, :] = rest - dot(side, strip, 1, 0, HIGHEST)
        if not chol:
            work[at:end, :] = strip


def identity(size):
    row = lax.broadcasted_iota(jnp.int32, (size, size), 0)
    return jnp.where(row == lax.broadcasted_iota(jnp.int32, (size, size), 1), 1.0, 0.0).astype(F32)


def strip_of(ref, start, count, at):
    return ref[pl.ds(start * WIDE + at, count, stride=WIDE), :]


def main_kernel(
    rows, cols, a_hbm, z_hbm,
    y_out, yt_out, x_out, xt_out, tk_out,
    v_out, vt_out, c_out, t_out, k_out, alin, zlin, a, z, panel, panel_t, gram, landed, g_out, top_out, rows_out, cols_out, work, w,
    v, v_half, v_sum, v_land, vt, vt_land, c, c_half, c_sum, c_land, c_row, t, t_land,
    *sems,
):
    sems = iter(sems)
    a_in = pltpu.make_async_copy(a_hbm, alin, next(sems))
    z_in = pltpu.make_async_copy(z_hbm, zlin, next(sems))
    a_in.start()
    z_in.start()
    p, q = lax.axis_index("row"), lax.axis_index("col")
    met = greet(rows, cols, p, q)
    first = q == 0
    chips = cols // 2
    my_z, core = q // 2, lax.rem(q, 2)
    other = 2 * my_z + 1 - core
    height, band = panel.shape
    slab, piece = rows_out.shape[1], top_out.shape[1]

    a_in.wait()
    row = lax.broadcasted_iota(jnp.int32, (height, 128), 0)
    for at in range(band // 128):
        panel[:, 128 * at : 128 * (at + 1)] = jnp.where((row < band) & (p == 0), 0.0, strip_of(alin, 0, height, at))
    gram[...] = dot(panel[...], panel[...], 0, 0, HIGHEST).reshape(gram.shape)
    def top_piece(to):
        return panel.at[pl.ds(pl.multiple_of(to * piece, piece), piece), :]

    def row_piece(to):
        return panel.at[pl.ds(pl.multiple_of(to * slab, slab), slab), :]

    def fan(axis, size, me, src, dst):
        return Fan(axis, size, me, next(sems), next(sems), src, dst)

    def cut(axis, size, me, root, src, dst):
        return Scatter(axis, size, me, root, next(sems), next(sems), src, dst)

    def ring(at):
        return Chips(cols, q, next(sems), next(sems), next(sems), next(sems), at)

    tall, flat = slab // 2, piece // 2
    halves = [(pl.ds(0, tall), pl.ds(0, flat)), (pl.ds(tall, tall), pl.ds(flat, flat))]

    reduce = fan("row", rows, p, lambda to: gram.at[to], lambda at: landed.at[at])
    g_wide = fan("row", rows, p, lambda to: g_out.at[p], lambda at: g_out.at[at])
    t_wide = fan("row", rows, p, lambda to: top_out.at[p], lambda at: top_out.at[at])
    c_wide = fan("row", rows, p, lambda to: cols_out.at[p], lambda at: cols_out.at[at])
    vt_cut = [
        fan("row", rows, p, lambda to, part=part: vt.at[to, part], lambda at, part=part: vt_land.at[at, part])
        for _, part in halves
    ]
    pt_cut = fan("row", rows, p, lambda to: t.at[to], lambda at: t_land.at[at])
    pc_wide = fan("row", rows, p, lambda to: c_row.at[p], lambda at: c_row.at[at])
    vt_all = [
        fan("row", rows, p, lambda to, part=part: vt_out.at[p, part], lambda at, part=part: vt_out.at[at, part])
        for _, part in halves
    ]
    pt_all = fan("row", rows, p, lambda to: t_out.at[p], lambda at: t_out.at[at])
    g_down = cut("col", cols, q, 0, lambda to: g_out.at[p], lambda to: g_out.at[p])
    t_cut = cut("row", rows, p, 1, top_piece, lambda to: top_out.at[to])
    t_down = cut("col", cols, q, 0, lambda to: top_out.at[p], lambda to: top_out.at[p])
    r_cut = cut("col", cols, q, 0, row_piece, lambda to: rows_out.at[to])
    c_cut = cut("row", rows, p, 0, lambda to: panel_t.at[to], lambda to: cols_out.at[to])
    r_wide, c_all = ring(lambda i: rows_out.at[i]), ring(lambda i: c_out.at[i])
    v_all = [ring(lambda i, part=part: v_out.at[i, part]) for part, _ in halves]

    met()

    @pl.when(first)
    def _():
        reduce.start()

        @pl.when(p == 1)
        def _():
            t_cut.start()

        r_cut.start()

    @pl.when(p == 0)
    def _():
        for at in range(WIDE):
            part = strip_of(alin, 0, band, at)
            if at < band // 128:
                part = jnp.where(q == 0, 0.0, part)
            panel_t[:, :, 128 * at : 128 * (at + 1)] = part.reshape(rows, band // rows, 128)
        c_cut.start()

    @pl.when(first)
    def _():
        landed[p] = gram[p]
        rows_out[0] = panel[:slab, :]

        @pl.when(p == 1)
        def _():
            top_out[1] = panel[piece : 2 * piece, :]

        reduce.wait_recv()
        g_out[p] = total(landed)
        g_down.start()

    @pl.when(p == 0)
    def _():
        cols_out[0] = panel_t[0]

    @pl.when(jnp.logical_not(first))
    def _():
        g_down.wait_recv()

    g_wide.start()

    @pl.when(jnp.logical_not(first))
    def _():
        r_cut.wait_recv()

    r_wide.start()

    @pl.when(p != 0)
    def _():
        c_cut.wait_recv()

    c_wide.start()

    @pl.when(first)
    def _():
        @pl.when(p != 1)
        def _():
            t_cut.wait_recv()

        t_down.start()

    @pl.when(jnp.logical_not(first))
    def _():
        t_down.wait_recv()

    t_wide.start()
    z_in.wait()
    for at in range(WIDE):
        a[:, 128 * at : 128 * (at + 1)] = strip_of(alin, 0, height, at)
        z[:, 128 * at : 128 * (at + 1)] = strip_of(zlin, 0, z.shape[0], at)
    g_wide.wait_recv()

    cholesky_inverse(g_out[...].reshape(band, band), work, w)
    r_wide.relay()

    def along(src, land, part):
        ss, rs = next(sems), next(sems)

        def copy(k):
            to = lax.rem(my_z + 1 + k, chips)
            return send(src.at[to, part], land.at[my_z, part], ss.at[k], rs.at[my_z], "col", 2 * to + core)

        def recv(k):
            at = lax.rem(my_z + 1 + k, chips)
            send(src.at[at, part], land.at[at, part], ss.at[k], rs.at[at], "col", 2 * at + core).wait_recv()

        return copy, recv

    c_wide.wait_recv()
    yt_out[...] = dot(w[...], cols_out[...].reshape(band, height), 1, 0)

    @pl.when(q == 1)
    def _():
        yt_out[:, :band] = yt_out[:, :band] + identity(band)

    image = dot(a[...], yt_out[...], 1, 1)
    for i in range(cols):
        v[i % 2, i // 2] = image[i * slab : (i + 1) * slab, :]
    v_swap = send(v.at[1 - core], v_half, next(sems), next(sems), "col", other)
    v_along = [along(v_sum, v_land, part) for part, _ in halves]
    c_swap = send(c.at[1 - core], c_half, next(sems), next(sems), "col", other)
    c_copy, c_recv = along(c_sum, c_land, pl.ds(0, piece))
    v_swap.start()
    r_wide.finish()
    y_out[...] = dot(rows_out[...].reshape(height, band), w[...], 1, 1)

    @pl.when(p == 1)
    def _():
        y_out[:band, :] = y_out[:band, :] + identity(band)

    v_swap.wait_recv()

    def v_add(i):
        v_sum[i] = v[core, i] + v_half[i]

    loop(chips, v_add)
    loop(chips - 1, lambda k: v_along[0][0](k).start())
    inner = dot(y_out[...], image, 0, 0)
    for i in range(cols):
        c[i % 2, i // 2] = inner[i * piece : (i + 1) * piece, :]
    c_swap.start()
    vt[...] = dot(y_out[...], a[...], 0, 0).reshape(vt.shape)
    vt_cut[0].start()
    c_swap.wait_recv()

    def c_add(i):
        c_sum[i] = c[core, i] + c_half[i]

    loop(chips, c_add)
    loop(chips - 1, lambda k: c_copy(k).start())
    loop(chips - 1, lambda k: v_along[1][0](k).start())
    vt_cut[1].start()
    t[...] = dot(z[...], y_out[...], 1, 0).reshape(t.shape)
    vt_land[p] = vt[p]
    t_land[p] = t[p]
    v_land[my_z] = v_sum[my_z]
    c_land[my_z] = c_sum[my_z]

    def send_v(n):
        loop(chips - 1, v_along[n][1])
        v_out[q, halves[n][0]] = total(v_land.at[:, halves[n][0]])
        v_all[n].start()

    def send_vt(n):
        vt_cut[n].wait_recv()
        vt_out[p, halves[n][1]] = total(vt_land.at[:, halves[n][1]])
        vt_all[n].start()

    def send_c():
        loop(chips - 1, c_recv)
        c_row[p] = total(c_land)
        pc_wide.start()
        pt_cut.start()

    def share_c():
        pc_wide.wait_recv()
        c_out[q] = total(c_row)
        c_all.start()

    t_wide.wait_recv()
    k_out[...] = identity(band) + dot(top_out[...].reshape(band, band), w[...], 1, 1, HIGHEST)
    eliminate(
        k_out, None, False, [(3, send_c), (5, lambda: send_v(0)), (6, lambda: send_vt(0)), (7, share_c)]
    )
    send_v(1)
    send_vt(1)
    pt_cut.wait_recv()
    t_out[p] = total(t_land)
    pt_all.start()
    v_all[0].relay()
    c_all.relay()
    v_all[1].relay()

    vt_all[0].wait_recv()
    vt_all[1].wait_recv()
    c_all.finish()
    inner_half = 0.5 * dot(dot(k_out[...], c_out[...].reshape(band, band), 0, 0), k_out[...], 1, 0)
    xt_out[...] = dot(k_out[...], vt_out[...].reshape(band, height), 0, 0) - dot(inner_half, yt_out[...], 0, 0)
    x_out[...] = dot(y_out[...], inner_half, 1, 0)
    pt_all.wait_recv()
    tk_out[...] = dot(t_out[...].reshape(tk_out.shape), k_out[...], 1, 0)
    v_all[0].finish()
    v_all[1].finish()
    x_out[...] = dot(v_out[...].reshape(height, band), k_out[...], 1, 0) - x_out[...]

    @pl.when(first)
    def _():
        reduce.wait_send()

        @pl.when(p == 1)
        def _():
            t_cut.wait_send()

        r_cut.wait_send()
        g_down.wait_send()
        t_down.wait_send()

    @pl.when(p == 0)
    def _():
        c_cut.wait_send()

    v_swap.wait_send()
    c_swap.wait_send()
    for copy, _ in v_along:
        loop(chips - 1, lambda k, copy=copy: copy(k).wait_send())
    loop(chips - 1, lambda k: c_copy(k).wait_send())
    for done in (g_wide, t_wide, c_wide, *vt_cut, pt_cut, pc_wide, *vt_all, pt_all):
        done.wait_send()


def main(rows, cols, band, alin, zlin):
    height = alin.shape[0] // WIDE
    count = zlin.shape[0] // WIDE
    chips, slab, piece, tp = cols // 2, height // cols, band // cols, count // rows
    dma = pltpu.SemaphoreType.DMA
    fan = [dma((rows,))] * 2
    cut = [dma((rows,)), dma]
    ring = [dma((chips,))] * 4
    half = [dma((chips,))] * 2
    vmem = pl.BlockSpec(memory_space=pltpu.VMEM)
    flat = (height, band)
    small = (rows, piece, band)
    outs = [flat, (band, height), flat, (band, height), (count, band)]
    scratch = [
        (cols, slab, band), (rows, piece, height), (cols, piece, band), (rows, tp, band), (band, band), alin.shape, zlin.shape, (height, height), (count, height), flat, (rows, piece, height), small, small, small, small,
        (cols, slab, band), (rows, piece, height), (band, band), (band, band),
        (2, chips, slab, band), (chips, slab, band), (chips, slab, band), (chips, slab, band),
        (rows, piece, height), (rows, piece, height),
        (2, chips, piece, band), (chips, piece, band), (chips, piece, band), (chips, piece, band), small,
        (rows, tp, band), (rows, tp, band),
    ]
    return pl.pallas_call(
        functools.partial(main_kernel, rows, cols),
        out_shape=tuple(jax.ShapeDtypeStruct(s, F32) for s in outs),
        in_specs=[pl.BlockSpec(memory_space=pltpu.HBM)] * 2,
        out_specs=(vmem,) * len(outs),
        scratch_shapes=[pltpu.VMEM(s, F32) for s in scratch] + [dma] * 2 + fan * 11 + cut * 5 + ring * 4 + [dma] * 2 + half * 2 + [dma] * 2 + half,
        compiler_params=pltpu.CompilerParams(collective_id=0, has_side_effects=True, vmem_limit_bytes=50 * 2**20),
        name="main",
    )(alin, zlin)


def update_kernel(alin, zlin, y, yt, x, xt, tk, a_hbm, z_hbm, a_out, z_out, sems):
    height, band = y.shape
    count = zlin.shape[0] // WIDE
    copies = []

    def put(src, dst, lines, n):
        copies.append(pltpu.make_async_copy(src.at[lines, :], dst.at[lines, :], sems.at[n]))
        copies[-1].start()

    parts = height // band
    for n in range(parts):
        lo = n * band
        block = slice(lo, lo + band)
        move = dot(x[block, :], yt[...], 1, 0) + dot(y[block, :], xt[...], 1, 0)
        for at in range(WIDE):
            lines = pl.ds(lo * WIDE + at, band, stride=WIDE)
            a_out[lines, :] = alin[lines, :] - move[:, 128 * at : 128 * (at + 1)]
        put(a_out, a_hbm, pl.ds(lo * WIDE, band * WIDE), n)
    turn = dot(tk[...], y[...], 1, 1)
    for at in range(WIDE):
        lines = pl.ds(at, count, stride=WIDE)
        z_out[lines, :] = zlin[lines, :] - turn[:, 128 * at : 128 * (at + 1)]
    put(z_out, z_hbm, pl.ds(0, count * WIDE), parts)
    for copy in copies:
        copy.wait()


def update(alin, zlin, *rest):
    vmem = pl.BlockSpec(memory_space=pltpu.VMEM)
    height, band = rest[0].shape
    return pl.pallas_call(
        update_kernel,
        out_shape=(jax.ShapeDtypeStruct(alin.shape, F32), jax.ShapeDtypeStruct(zlin.shape, F32)),
        in_specs=[vmem] * (2 + len(rest)),
        out_specs=(pl.BlockSpec(memory_space=pltpu.HBM),) * 2,
        scratch_shapes=[
            pltpu.VMEM(alin.shape, F32),
            pltpu.VMEM(zlin.shape, F32),
            pltpu.SemaphoreType.DMA((height // band + 1,)),
        ],
        compiler_params=pltpu.CompilerParams(vmem_limit_bytes=24 * 2**20),
        name="update",
    )(alin, zlin, *rest)


def on_device(rows, cols, matrix, vectors):
    band = matrix.shape[2]
    alin = matrix.reshape(-1, 128)
    zlin = vectors.reshape(-1, 128)
    a, z = update(alin, zlin, *main(rows, cols, band, alin, zlin))
    return a.reshape(matrix.shape), z.reshape(vectors.shape)


def solution(mesh):
    specs = (P(None, "row", None, None, "col", None), P("col", None, "row", None))
    return jax.shard_map(
        functools.partial(on_device, mesh.shape["row"], mesh.shape["col"]),
        mesh=mesh,
        in_specs=specs,
        out_specs=specs,
        check_vma=False,
    )
```

```python
import functools

import jax
import jax.numpy as jnp
from jax import lax
from jax.experimental import pallas as pl
from jax.experimental.pallas import tpu as pltpu
from jax.sharding import PartitionSpec as P

MESH = pl.DeviceIdType.MESH
F32 = jnp.float32
HIGH = lax.Precision.HIGH
HIGHEST = lax.Precision.HIGHEST
STEP = 64
FINE = 32
GROUP = 16
WIDE = 6


def dot(a, b, ca, cb, precision=HIGH):
    return lax.dot_general(
        a, b, (((ca,), (cb,)), ((), ())), precision=precision, preferred_element_type=F32
    )


def send(src, dst, ssem, rsem, axis, to):
    return pltpu.make_async_remote_copy(
        src_ref=src, dst_ref=dst, send_sem=ssem, recv_sem=rsem, device_id={axis: to}, device_id_type=MESH
    )


def loop(n, body):
    lax.fori_loop(0, n, lambda k, c: (body(k), c)[1], 0)


def greet(rows, cols, p, q):
    barrier = pltpu.get_barrier_semaphore()

    def hello_row(k):
        pl.semaphore_signal(barrier, inc=1, device_id={"row": lax.rem(p + 1 + k, rows)}, device_id_type=MESH)

    def hello_col(k):
        pl.semaphore_signal(barrier, inc=1, device_id={"col": lax.rem(q + 1 + k, cols)}, device_id_type=MESH)

    loop(rows - 1, hello_row)
    loop(cols - 1, hello_col)
    return lambda: pl.semaphore_wait(barrier, rows + cols - 2)


class Fan:
    def __init__(self, axis, size, me, ssem, rsem, src, dst, recv=None):
        self.axis, self.size, self.me = axis, size, me
        self.ssem, self.rsem, self.src, self.dst = ssem, rsem, src, dst
        self.recv = recv

    def copy(self, k):
        to = lax.rem(self.me + 1 + k, self.size)
        return send(self.src(to), self.dst(self.me), self.ssem.at[k], self.rsem.at[self.me], self.axis, to)

    def start(self):
        loop(self.size - 1, lambda k: self.copy(k).start())

    def wait_recv(self):
        def one(k):
            at = lax.rem(self.me + 1 + k, self.size)
            ref = self.dst(at)
            send(ref, ref, self.ssem.at[k], self.rsem.at[at], self.axis, at).wait_recv()

        loop(self.size - 1, one)

    def wait_send(self):
        loop(self.size - 1, lambda k: self.copy(k).wait_send())


class Scatter:
    def __init__(self, axis, size, me, root, ssem, rsem, src, dst):
        self.axis, self.size, self.me, self.root = axis, size, me, root
        self.ssem, self.rsem, self.src, self.dst = ssem, rsem, src, dst

    def copy(self, k):
        to = lax.rem(self.me + 1 + k, self.size)
        return send(self.src(to), self.dst(to), self.ssem.at[k], self.rsem, self.axis, to)

    def start(self):
        loop(self.size - 1, lambda k: self.copy(k).start())

    def wait_recv(self):
        ref = self.dst(self.me)
        send(ref, ref, self.ssem.at[0], self.rsem, self.axis, self.root).wait_recv()

    def wait_send(self):
        loop(self.size - 1, lambda k: self.copy(k).wait_send())


class Chips:
    def __init__(self, cols, q, zs, zr, ss, sr, at):
        self.chips, self.cols, self.q, self.at = cols // 2, cols, q, at
        self.z, self.c = q // 2, lax.rem(q, 2)
        self.zs, self.zr, self.ss, self.sr = zs, zr, ss, sr

    def along(self, k):
        z = lax.rem(self.z + 1 + k, self.chips)
        mine = self.at(self.q)
        return send(mine, mine, self.zs.at[k], self.zr.at[self.z], "col", 2 * z + self.c)

    def across(self, z):
        piece = self.at(2 * z + self.c)
        return send(piece, piece, self.ss.at[z], self.sr.at[z], "col", 2 * self.z + 1 - self.c)

    def start(self):
        loop(self.chips - 1, lambda k: self.along(k).start())
        self.across(self.z).start()

    def relay(self):
        def one(k):
            z = lax.rem(self.z + 1 + k, self.chips)
            piece = self.at(2 * z + self.c)
            send(piece, piece, self.zs.at[k], self.zr.at[z], "col", 2 * z + self.c).wait_recv()
            self.across(z).start()

        loop(self.chips - 1, one)

    def finish(self):
        loop(self.chips - 1, lambda k: self.along(k).wait_send())

        def one(z):
            self.across(z).wait_send()
            piece = self.at(2 * z + 1 - self.c)
            send(piece, piece, self.ss.at[z], self.sr.at[z], "col", 2 * self.z + 1 - self.c).wait_recv()

        loop(self.chips, one)


def total(ref):
    size = ref.shape[0]
    acc = ref[0]
    for i in range(1, size):
        acc = acc + ref[i]
    return acc


def splat_row(x, j):
    return jnp.broadcast_to(x[j : j + 1, :], x.shape)


def small_factor(tile, off):
    row = lax.broadcasted_iota(jnp.int32, tile.shape, 0)
    lane = lax.broadcasted_iota(jnp.int32, tile.shape, 1)
    inverse = jnp.where(row == lane, 1.0, 0.0).astype(F32)
    done, pivots = [], []
    for g in range(0, STEP, GROUP):
        cols = [jnp.broadcast_to(tile[:, off + g + i : off + g + i + 1], tile.shape) for i in range(GROUP)]
        row = lax.broadcasted_iota(jnp.int32, tile.shape, 0)
        for i in range(0, GROUP, 2):
            here, there = cols[i], cols[i + 1]
            a, b, d = splat_row(here, i), splat_row(there, i), splat_row(there, i + 1)
            det = a * d - b * b
            over_a, over_det = 1.0 / a, 1.0 / det
            pivots += [a[:1, :], (det * over_a)[:1, :]]
            m0 = jnp.where(row > i + 1, (here * d - there * b) * over_det, jnp.where(row == i + 1, b * over_a, 0.0))
            m1 = jnp.where(row > i + 1, (there * a - here * b) * over_det, 0.0)
            for k in range(i + 2, GROUP):
                cols[k] = cols[k] - m0 * splat_row(cols[k], i) - m1 * splat_row(cols[k], i + 1)
            if g + GROUP < STEP:
                tile = tile - m0 * splat_row(tile, i) - m1 * splat_row(tile, i + 1)
            inverse = inverse - m0 * splat_row(inverse, i) - m1 * splat_row(inverse, i + 1)
        done.append(inverse[:GROUP, :])
        tile, inverse = tile[GROUP:, :], inverse[GROUP:, :]
    inverse = jnp.concatenate(done, axis=0) * lax.rsqrt(jnp.concatenate(pivots, axis=0))
    return inverse[:, :STEP]


def small_inverse(tile, off):
    row = lax.broadcasted_iota(jnp.int32, tile.shape, 0)
    lane = lax.broadcasted_iota(jnp.int32, tile.shape, 1)
    inverse = jnp.where(row == lane, 1.0, 0.0).astype(F32)
    for g in range(0, FINE, GROUP):
        cols = [jnp.broadcast_to(tile[:, off + g + i : off + g + i + 1], tile.shape) for i in range(GROUP)]
        for i in range(GROUP):
            j = g + i
            scale = 1.0 / splat_row(cols[i], j)
            m = jnp.where(row == j, 1.0 - scale, cols[i] * scale)
            for k in range(i + 1, GROUP):
                cols[k] = cols[k] - m * splat_row(cols[k], j)
            tile = tile - m * splat_row(tile, j)
            inverse = inverse - m * splat_row(inverse, j)
    return inverse[:, :FINE]


def cholesky_inverse(gram, work, out, between=()):
    size = gram.shape[0]
    diagonal = jnp.where(identity(size) > 0.0, gram, 0.0)
    across = lax.rsqrt(jnp.sum(diagonal, axis=0, keepdims=True))
    work[...] = gram * across * lax.rsqrt(jnp.sum(diagonal, axis=1, keepdims=True))
    eliminate(work, out, True, between)
    out[...] = out[...] * across


def eliminate(work, out, chol, between=()):
    size = work.shape[0]
    step = STEP if chol else FINE
    lane = lax.broadcasted_iota(jnp.int32, (step, size), 1)
    row = lax.broadcasted_iota(jnp.int32, (step, size), 0)
    for at in range(0, size, step):
        end = at + step
        for when, act in between:
            if when == at // step:
                act()
        base = at // 128 * 128
        tile = work[at:end, base : base + 128]
        inverse = small_factor(tile, at - base) if chol else small_inverse(tile, at - base)
        strip = jnp.where(
            (lane >= at) & (lane < end), jnp.where(lane - at == row, 1.0, 0.0), work[at:end, :]
        )
        strip = dot(inverse, strip, 1, 0, HIGHEST)
        if chol:
            out[at:end, :] = jnp.where(lane < end, strip, 0.0)
            spans = [(end, size)]
        else:
            spans = [(0, at), (end, size)]
        for lo, hi in spans:
            if lo == hi:
                continue
            side = work[lo:hi, at:end]
            if chol:
                side = dot(side, inverse, 1, 1, HIGHEST)
            wide = lax.broadcasted_iota(jnp.int32, (hi - lo, size), 1)
            rest = jnp.where((wide >= at) & (wide < end), 0.0, work[lo:hi, :])
            work[lo:hi, :] = rest - dot(side, strip, 1, 0, HIGHEST)
        if not chol:
            work[at:end, :] = strip


def identity(size):
    row = lax.broadcasted_iota(jnp.int32, (size, size), 0)
    return jnp.where(row == lax.broadcasted_iota(jnp.int32, (size, size), 1), 1.0, 0.0).astype(F32)


def strip_of(ref, start, count, at):
    return ref[pl.ds(start * WIDE + at, count, stride=WIDE), :]


def main_kernel(
    rows, cols, a_hbm, z_hbm,
    y_out, yt_out, x_out, xt_out, tk_out,
    v_out, vt_out, c_out, t_out, k_out, alin, zlin, a, z, panel, panel_t, gram, landed, g_out, top_out, rows_out, cols_out, work, w,
    v, v_half, v_sum, v_land, vt, vt_land, c, c_half, c_sum, c_land, c_row, t, t_land,
    *sems,
):
    sems = iter(sems)
    a_in = pltpu.make_async_copy(a_hbm, alin, next(sems))
    z_in = pltpu.make_async_copy(z_hbm, zlin, next(sems))
    a_in.start()
    z_in.start()
    p, q = lax.axis_index("row"), lax.axis_index("col")
    met = greet(rows, cols, p, q)
    first = q == 0
    chips = cols // 2
    my_z, core = q // 2, lax.rem(q, 2)
    other = 2 * my_z + 1 - core
    height, band = panel.shape
    slab, piece = rows_out.shape[1], top_out.shape[1]

    a_in.wait()
    row = lax.broadcasted_iota(jnp.int32, (height, 128), 0)
    for at in range(band // 128):
        panel[:, 128 * at : 128 * (at + 1)] = jnp.where((row < band) & (p == 0), 0.0, strip_of(alin, 0, height, at))
    gram[...] = dot(panel[...], panel[...], 0, 0, HIGHEST).reshape(gram.shape)
    def top_piece(to):
        return panel.at[pl.ds(pl.multiple_of(to * piece, piece), piece), :]

    def row_piece(to):
        return panel.at[pl.ds(pl.multiple_of(to * slab, slab), slab), :]

    def fan(axis, size, me, src, dst):
        return Fan(axis, size, me, next(sems), next(sems), src, dst)

    def cut(axis, size, me, root, src, dst):
        return Scatter(axis, size, me, root, next(sems), next(sems), src, dst)

    def ring(at):
        return Chips(cols, q, next(sems), next(sems), next(sems), next(sems), at)

    tall, flat = slab // 2, piece // 2
    halves = [(pl.ds(0, tall), pl.ds(0, flat)), (pl.ds(tall, tall), pl.ds(flat, flat))]

    reduce = fan("row", rows, p, lambda to: gram.at[to], lambda at: landed.at[at])
    g_wide = fan("row", rows, p, lambda to: g_out.at[p], lambda at: g_out.at[at])
    t_wide = fan("row", rows, p, lambda to: top_out.at[p], lambda at: top_out.at[at])
    c_wide = fan("row", rows, p, lambda to: cols_out.at[p], lambda at: cols_out.at[at])
    vt_cut = [
        fan("row", rows, p, lambda to, part=part: vt.at[to, part], lambda at, part=part: vt_land.at[at, part])
        for _, part in halves
    ]
    pt_cut = fan("row", rows, p, lambda to: t.at[to], lambda at: t_land.at[at])
    pc_wide = fan("row", rows, p, lambda to: c_row.at[p], lambda at: c_row.at[at])
    vt_all = [
        fan("row", rows, p, lambda to, part=part: vt_out.at[p, part], lambda at, part=part: vt_out.at[at, part])
        for _, part in halves
    ]
    pt_all = fan("row", rows, p, lambda to: t_out.at[p], lambda at: t_out.at[at])
    g_down = cut("col", cols, q, 0, lambda to: g_out.at[p], lambda to: g_out.at[p])
    t_cut = cut("row", rows, p, 1, top_piece, lambda to: top_out.at[to])
    t_down = cut("col", cols, q, 0, lambda to: top_out.at[p], lambda to: top_out.at[p])
    r_cut = cut("col", cols, q, 0, row_piece, lambda to: rows_out.at[to])
    c_cut = cut("row", rows, p, 0, lambda to: panel_t.at[to], lambda to: cols_out.at[to])
    r_wide, c_all = ring(lambda i: rows_out.at[i]), ring(lambda i: c_out.at[i])
    v_all = [ring(lambda i, part=part: v_out.at[i, part]) for part, _ in halves]

    met()

    @pl.when(first)
    def _():
        reduce.start()

        @pl.when(p == 1)
        def _():
            t_cut.start()

        r_cut.start()

    @pl.when(p == 0)
    def _():
        for at in range(WIDE):
            part = strip_of(alin, 0, band, at)
            if at < band // 128:
                part = jnp.where(q == 0, 0.0, part)
            panel_t[:, :, 128 * at : 128 * (at + 1)] = part.reshape(rows, band // rows, 128)
        c_cut.start()

    @pl.when(first)
    def _():
        landed[p] = gram[p]
        rows_out[0] = panel[:slab, :]

        @pl.when(p == 1)
        def _():
            top_out[1] = panel[piece : 2 * piece, :]

        reduce.wait_recv()
        g_out[p] = total(landed)
        g_down.start()

        @pl.when(p != 1)
        def _():
            t_cut.wait_recv()

        t_down.start()

    @pl.when(p == 0)
    def _():
        cols_out[0] = panel_t[0]

    @pl.when(jnp.logical_not(first))
    def _():
        g_down.wait_recv()

    g_wide.start()

    @pl.when(jnp.logical_not(first))
    def _():
        r_cut.wait_recv()

    r_wide.start()

    @pl.when(p != 0)
    def _():
        c_cut.wait_recv()

    c_wide.start()

    z_in.wait()
    for at in range(WIDE):
        a[:, 128 * at : 128 * (at + 1)] = strip_of(alin, 0, height, at)
        z[:, 128 * at : 128 * (at + 1)] = strip_of(zlin, 0, z.shape[0], at)
    g_wide.wait_recv()

    def meanwhile():
        r_wide.relay()

        @pl.when(jnp.logical_not(first))
        def _():
            t_down.wait_recv()

        t_wide.start()

    cholesky_inverse(g_out[...].reshape(band, band), work, w, [(band // STEP // 2, meanwhile)])

    def along(src, land, part):
        ss, rs = next(sems), next(sems)

        def copy(k):
            to = lax.rem(my_z + 1 + k, chips)
            return send(src.at[to, part], land.at[my_z, part], ss.at[k], rs.at[my_z], "col", 2 * to + core)

        def recv(k):
            at = lax.rem(my_z + 1 + k, chips)
            send(src.at[at, part], land.at[at, part], ss.at[k], rs.at[at], "col", 2 * at + core).wait_recv()

        return copy, recv

    c_wide.wait_recv()
    yt_out[...] = dot(w[...], cols_out[...].reshape(band, height), 1, 0)

    @pl.when(q == 1)
    def _():
        yt_out[:, :band] = yt_out[:, :band] + identity(band)

    image = dot(a[...], yt_out[...], 1, 1)
    for i in range(cols):
        v[i % 2, i // 2] = image[i * slab : (i + 1) * slab, :]
    v_swap = send(v.at[1 - core], v_half, next(sems), next(sems), "col", other)
    v_along = [along(v_sum, v_land, part) for part, _ in halves]
    c_swap = send(c.at[1 - core], c_half, next(sems), next(sems), "col", other)
    c_copy, c_recv = along(c_sum, c_land, pl.ds(0, piece))
    v_swap.start()
    r_wide.finish()
    y_out[...] = dot(rows_out[...].reshape(height, band), w[...], 1, 1)

    @pl.when(p == 1)
    def _():
        y_out[:band, :] = y_out[:band, :] + identity(band)

    v_swap.wait_recv()

    def v_add(i):
        v_sum[i] = v[core, i] + v_half[i]

    loop(chips, v_add)
    loop(chips - 1, lambda k: v_along[0][0](k).start())
    inner = dot(y_out[...], image, 0, 0)
    for i in range(cols):
        c[i % 2, i // 2] = inner[i * piece : (i + 1) * piece, :]
    c_swap.start()
    vt[...] = dot(y_out[...], a[...], 0, 0).reshape(vt.shape)
    vt_cut[0].start()
    c_swap.wait_recv()

    def c_add(i):
        c_sum[i] = c[core, i] + c_half[i]

    loop(chips, c_add)
    loop(chips - 1, lambda k: c_copy(k).start())
    loop(chips - 1, lambda k: v_along[1][0](k).start())
    vt_cut[1].start()
    t[...] = dot(z[...], y_out[...], 1, 0).reshape(t.shape)
    pt_cut.start()
    vt_land[p] = vt[p]
    t_land[p] = t[p]
    v_land[my_z] = v_sum[my_z]
    c_land[my_z] = c_sum[my_z]

    def send_v(n):
        loop(chips - 1, v_along[n][1])
        v_out[q, halves[n][0]] = total(v_land.at[:, halves[n][0]])
        v_all[n].start()

    def send_vt(n):
        vt_cut[n].wait_recv()
        vt_out[p, halves[n][1]] = total(vt_land.at[:, halves[n][1]])
        vt_all[n].start()

    def send_c():
        loop(chips - 1, c_recv)
        c_row[p] = total(c_land)
        pc_wide.start()

    def share_c():
        pc_wide.wait_recv()
        c_out[q] = total(c_row)
        c_all.start()

    t_wide.wait_recv()
    k_out[...] = identity(band) + dot(top_out[...].reshape(band, band), w[...], 1, 1, HIGHEST)
    eliminate(
        k_out, None, False, [(4, send_c), (5, lambda: send_v(0)), (7, lambda: send_vt(0))]
    )
    send_v(1)
    share_c()
    send_vt(1)
    pt_cut.wait_recv()
    t_out[p] = total(t_land)
    pt_all.start()
    v_all[0].relay()
    v_all[1].relay()
    c_all.relay()

    vt_all[0].wait_recv()
    vt_all[1].wait_recv()
    c_all.finish()
    inner_half = 0.5 * dot(dot(k_out[...], c_out[...].reshape(band, band), 0, 0), k_out[...], 1, 0)
    xt_out[...] = dot(k_out[...], vt_out[...].reshape(band, height), 0, 0) - dot(inner_half, yt_out[...], 0, 0)
    x_out[...] = dot(y_out[...], inner_half, 1, 0)
    pt_all.wait_recv()
    tk_out[...] = dot(t_out[...].reshape(tk_out.shape), k_out[...], 1, 0)
    v_all[0].finish()
    v_all[1].finish()
    x_out[...] = dot(v_out[...].reshape(height, band), k_out[...], 1, 0) - x_out[...]

    @pl.when(first)
    def _():
        reduce.wait_send()

        @pl.when(p == 1)
        def _():
            t_cut.wait_send()

        r_cut.wait_send()
        g_down.wait_send()
        t_down.wait_send()

    @pl.when(p == 0)
    def _():
        c_cut.wait_send()

    v_swap.wait_send()
    c_swap.wait_send()
    for copy, _ in v_along:
        loop(chips - 1, lambda k, copy=copy: copy(k).wait_send())
    loop(chips - 1, lambda k: c_copy(k).wait_send())
    for done in (g_wide, t_wide, c_wide, *vt_cut, pt_cut, pc_wide, *vt_all, pt_all):
        done.wait_send()


def main(rows, cols, band, alin, zlin):
    height = alin.shape[0] // WIDE
    count = zlin.shape[0] // WIDE
    chips, slab, piece, tp = cols // 2, height // cols, band // cols, count // rows
    dma = pltpu.SemaphoreType.DMA
    fan = [dma((rows,))] * 2
    cut = [dma((rows,)), dma]
    ring = [dma((chips,))] * 4
    half = [dma((chips,))] * 2
    vmem = pl.BlockSpec(memory_space=pltpu.VMEM)
    flat = (height, band)
    small = (rows, piece, band)
    outs = [flat, (band, height), flat, (band, height), (count, band)]
    scratch = [
        (cols, slab, band), (rows, piece, height), (cols, piece, band), (rows, tp, band), (band, band), alin.shape, zlin.shape, (height, height), (count, height), flat, (rows, piece, height), small, small, small, small,
        (cols, slab, band), (rows, piece, height), (band, band), (band, band),
        (2, chips, slab, band), (chips, slab, band), (chips, slab, band), (chips, slab, band),
        (rows, piece, height), (rows, piece, height),
        (2, chips, piece, band), (chips, piece, band), (chips, piece, band), (chips, piece, band), small,
        (rows, tp, band), (rows, tp, band),
    ]
    return pl.pallas_call(
        functools.partial(main_kernel, rows, cols),
        out_shape=tuple(jax.ShapeDtypeStruct(s, F32) for s in outs),
        in_specs=[pl.BlockSpec(memory_space=pltpu.HBM)] * 2,
        out_specs=(vmem,) * len(outs),
        scratch_shapes=[pltpu.VMEM(s, F32) for s in scratch] + [dma] * 2 + fan * 11 + cut * 5 + ring * 4 + [dma] * 2 + half * 2 + [dma] * 2 + half,
        compiler_params=pltpu.CompilerParams(collective_id=0, has_side_effects=True, vmem_limit_bytes=50 * 2**20),
        name="main",
    )(alin, zlin)


def update_kernel(alin, zlin, y, yt, x, xt, tk, a_hbm, z_hbm, a_out, z_out, sems):
    height, band = y.shape
    count = zlin.shape[0] // WIDE
    copies = []

    def put(src, dst, lines, n):
        copies.append(pltpu.make_async_copy(src.at[lines, :], dst.at[lines, :], sems.at[n]))
        copies[-1].start()

    parts = height // band
    for n in range(parts):
        lo = n * band
        block = slice(lo, lo + band)
        move = dot(x[block, :], yt[...], 1, 0) + dot(y[block, :], xt[...], 1, 0)
        for at in range(WIDE):
            lines = pl.ds(lo * WIDE + at, band, stride=WIDE)
            a_out[lines, :] = alin[lines, :] - move[:, 128 * at : 128 * (at + 1)]
        put(a_out, a_hbm, pl.ds(lo * WIDE, band * WIDE), n)
    turn = dot(tk[...], y[...], 1, 1)
    for at in range(WIDE):
        lines = pl.ds(at, count, stride=WIDE)
        z_out[lines, :] = zlin[lines, :] - turn[:, 128 * at : 128 * (at + 1)]
    put(z_out, z_hbm, pl.ds(0, count * WIDE), parts)
    for copy in copies:
        copy.wait()


def update(alin, zlin, *rest):
    vmem = pl.BlockSpec(memory_space=pltpu.VMEM)
    height, band = rest[0].shape
    return pl.pallas_call(
        update_kernel,
        out_shape=(jax.ShapeDtypeStruct(alin.shape, F32), jax.ShapeDtypeStruct(zlin.shape, F32)),
        in_specs=[vmem] * (2 + len(rest)),
        out_specs=(pl.BlockSpec(memory_space=pltpu.HBM),) * 2,
        scratch_shapes=[
            pltpu.VMEM(alin.shape, F32),
            pltpu.VMEM(zlin.shape, F32),
            pltpu.SemaphoreType.DMA((height // band + 1,)),
        ],
        compiler_params=pltpu.CompilerParams(vmem_limit_bytes=24 * 2**20),
        name="update",
    )(alin, zlin, *rest)


def on_device(rows, cols, matrix, vectors):
    band = matrix.shape[2]
    alin = matrix.reshape(-1, 128)
    zlin = vectors.reshape(-1, 128)
    a, z = update(alin, zlin, *main(rows, cols, band, alin, zlin))
    return a.reshape(matrix.shape), z.reshape(vectors.shape)


def solution(mesh):
    specs = (P(None, "row", None, None, "col", None), P("col", None, "row", None))
    return jax.shard_map(
        functools.partial(on_device, mesh.shape["row"], mesh.shape["col"]),
        mesh=mesh,
        in_specs=specs,
        out_specs=specs,
        check_vma=False,
    )
```
